128 devices in a mesh: slab: 32 (over z, y, core), row: 4 (over x).
Axes of the slice: x: 4, y: 4, z: 4, core: 2. Of those that a mesh axis runs over, the one named last changes fastest.
Arguments:
- voltage: float32 [512, 98304], P(None, ('slab', 'row')), may hold values from -6 to 6
- potential: float32 [256, 512, 256], P('slab', 'row'), may hold values from -6 to 6
- transfer: float32 [128, 512], replicated, may hold values from -0.25 to 0.25
- conductance: float32 [512], replicated, may hold values from 0.2 to 2
- inverses: float32 [8, 64, 64], replicated, may hold values from -1 to 1
- parents: int32 [7], replicated, may hold values from 0 to 6, as said below
- target: int32 [98304, 1], P(('slab', 'row')), may hold values from 0 to 127; in each aligned block of 768 rows (0 to 767, 768 to 1535, ...) at most 12 rows name the same one
- place: int32 [98304], P(('slab', 'row')), may hold values from 0 to 2047
Outputs:
- voltage_out: float32 [512, 98304], P(None, ('slab', 'row'))
- potential_out: float32 [256, 512, 256], P('slab', 'row')
The draws below stay inside these ranges and needn't reach their ends.
Inputs may be any that keep to these rules, and one draw needn't show every extreme that they name: `target`: among the 768 cells of one device, at most 12 name the same owner; in every draw some owner is named by exactly 12 of one device's cells. `parents`: entry k is smaller than k + 1; the last entry is 6.
All inputs are finite; a program needn't handle non-finite values.
Results may differ from the reference program's by a relative error of at most 0.00011.
Values sent between devices are 32-bit elements; how exact they have to be, the bound alone decides.
A program may use at most 64 MiB of HBM per device.

```python
import math
import jax
import jax.numpy as jnp
import numpy as np
from jax import lax

COMP = 512
BS = 64
NB = 8
CELLS_DEV = 768
CELLS = 98304
CAP = 12
CZ = 8
CY = 128
GX = 256
PT = 128
NPOS = 2048
NZ = 256
NY = 512
STEPS = 2
SWEEPS = 4
N_SLAB = 32
N_ROW = 4


def draw_inverses(key, part):
    noise = jax.random.truncated_normal(key, -4.0, 4.0, (NB, BS, BS), jnp.float32)
    return 0.6 * jnp.eye(BS, dtype=jnp.float32)[None] + 0.3 / math.sqrt(BS) * noise


def draw_parents(key, part):
    limits = jnp.arange(1, NB, dtype=jnp.int32)
    drawn = jax.random.randint(key, (NB - 1,), 0, limits, dtype=jnp.int32)
    counter = jnp.arange(NB - 1, dtype=jnp.int32)
    return jnp.where(counter == NB - 2, jnp.full_like(drawn, NB - 2), drawn).astype(jnp.int32)


def with_ends(result, rng, smallest, top_value):
    longest = result.shape.index(max(result.shape))
    spots = []
    for shift in (0, 1):
        where = [jax.random.randint(jax.random.fold_in(rng, axis), (), 0, length) for axis, length in enumerate(result.shape)]
        where[longest] = (where[longest] + shift) % result.shape[longest]
        spots.append(tuple(where))
    return result.at[spots[0]].set(smallest).at[spots[1]].set(top_value)


def block_levels(stream_key, shape, pieces, low, top_value):
    gain = 1.0
    for dim, shards_of in pieces:
        steps = jax.random.uniform(jax.random.fold_in(jax.random.fold_in(stream_key, 6), dim), (shards_of,), jnp.float32, low / len(pieces), top_value / len(pieces))
        gain = gain * jnp.repeat(jnp.exp(steps), shape[dim] // shards_of).reshape((-1,) + (1,) * (len(shape) - 1 - dim))
    return gain


def assign_block(rng, own, number, rows, amount, top, most, skew):
    ranking = jax.random.permutation(rng, amount)
    crowded, usual = load_shares(amount, rows * top, most, skew, True), load_shares(amount, rows * top, most, skew, False)
    places = jnp.arange(amount)

    def named(lengths, rotation):
        used = int((lengths > 0).sum())
        fixed = max(1, used // 4)
        moved = fixed + (places - fixed + rotation * (used - fixed)) % max(1, amount - fixed)
        return jnp.zeros((amount,), jnp.int32).at[ranking[jnp.where(places < fixed, places, moved)]].set(jnp.asarray(lengths, jnp.int32))

    lengths = jnp.where(number % 4 == 0, named(crowded, number // 4), named(usual, number - number // 4 - 1))
    mixed = jax.random.permutation(jax.random.fold_in(own, 3), amount)
    giver, taker = mixed[0:amount // 2 * 2:2], mixed[1:amount // 2 * 2:2]
    room = jnp.minimum(lengths[giver] - 1, most - lengths[taker]) // 2
    room = jnp.where((giver == ranking[0]) | (taker == ranking[0]) | (lengths[taker] == 0), 0, jnp.maximum(room, 0))
    moved = jax.random.randint(jax.random.fold_in(own, 4), (amount // 2,), 0, 1 << 20) % (room + 1)
    lengths = lengths.at[giver].add(-moved).at[taker].add(moved)
    items = jnp.searchsorted(jnp.cumsum(lengths), jnp.arange(rows * top), side="right").astype(jnp.int32)
    listing = items.reshape(top, rows).T
    listing = listing[jax.random.permutation(jax.random.fold_in(own, 1), rows)]
    rotation = jax.random.randint(jax.random.fold_in(own, 2), (rows, 1), 0, top)
    return jnp.take_along_axis(listing, (jnp.arange(top)[None, :] + rotation) % top, axis=1)


def load_shares(amount, total, most, lean, full):
    weights = [(1 << 20) // math.isqrt(rank ** lean) + 1 for rank in range(1, amount + 1)]
    largest = most if full else min(most, max(-(-total // amount), total * weights[0] // sum(weights)))
    least = 1 if total - largest >= amount - 1 else 0
    given, surplus = [largest] + [least] * (amount - 1), total - largest - least * (amount - 1)
    while surplus > 0:
        candidates = [i for i in range(1, amount) if given[i] < largest] or [i for i in range(1, amount) if given[i] < most]
        mass, budget = sum([weights[i] for i in candidates]), surplus
        for i in candidates:
            more = min(most - given[i], max(1, budget * weights[i] // mass), surplus)
            given[i] = given[i] + more
            surplus = surplus - more
    return np.array(given)


def gaussian(stream_key, shape, scale, limit, cuts=(), kind=jnp.bfloat16):
    factor_of = block_levels(stream_key, shape, cuts, -0.22, 0.18) if cuts else 1.0
    array = jax.random.normal(stream_key, shape, jnp.float32) * scale * factor_of
    return jnp.minimum(jnp.maximum(array, -limit), limit).astype(kind)


def setup_inputs(seed: int = 0) -> dict:
    key_of = jax.random.split(jax.random.key(seed), 9)
    voltage = gaussian(key_of[0], (COMP, CELLS), 1.0, 6.0, ((1, 128),), jnp.float32)
    potential = gaussian(key_of[1], (NZ, NY, GX), 1.0, 6.0, ((0, 32), (1, 4)), jnp.float32)
    transfer = gaussian(key_of[2], (PT, COMP), COMP ** -0.5, 0.25, (), jnp.float32)
    conductance = jnp.clip(jnp.exp(jax.random.uniform(key_of[3], (COMP,), jnp.float32, math.log(0.2), math.log(2.0))), 0.2, 2.0)
    inverses = draw_inverses(jax.random.fold_in(key_of[8], 71), 0)
    parents = draw_parents(jax.random.fold_in(key_of[8], 71), 0)
    target_keys = jax.random.split(jax.random.fold_in(key_of[6], 1), CELLS // CELLS_DEV)
    target_turns = jax.random.permutation(jax.random.fold_in(key_of[6], 3), CELLS // CELLS_DEV)
    target = jax.vmap(lambda own, number: assign_block(jax.random.fold_in(key_of[6], 2), own, number, CELLS_DEV, N_SLAB * N_ROW, 1, CAP, 1))(target_keys, target_turns).reshape((CELLS, 1))
    place = with_ends(jax.random.randint(key_of[7], (CELLS,), 0, NPOS), jax.random.fold_in(key_of[7], 1), 0, NPOS - 1).astype(jnp.int32)
    return dict(voltage=voltage, potential=potential, transfer=transfer, conductance=conductance, inverses=inverses, parents=parents, target=target, place=place)


screening = 0.25
coupling = 0.5


def hines_solve(rhs, inverses, parents):
    number = inverses.shape[0]
    width = inverses.shape[1]
    blocks = rhs.reshape(number, width, rhs.shape[1])
    solved = []
    for segment in range(number):
        right = blocks[segment]
        if segment > 0:
            above = jnp.zeros_like(right)
            for earlier in range(segment):
                above = above + jnp.where(parents[segment - 1] == earlier, solved[earlier], jnp.zeros_like(right))
            right = right + coupling * above
        solved.append(jnp.dot(inverses[segment], right, precision=lax.Precision.HIGHEST, preferred_element_type=jnp.float32))
    return jnp.concatenate(solved, axis=0)


def relax_grid(field, source):
    padded = jnp.pad(field, 1)
    beside = padded[2:, 1:-1, 1:-1] + padded[:-2, 1:-1, 1:-1]
    beside = beside + padded[1:-1, 2:, 1:-1] + padded[1:-1, :-2, 1:-1]
    beside = beside + padded[1:-1, 1:-1, 2:] + padded[1:-1, 1:-1, :-2]
    return (beside + source) / (6.0 + screening)


def reference(voltage, potential, transfer, conductance, inverses, parents, target, place):
    dev_count = N_SLAB * N_ROW
    patch_of = (target[:, 0] * NPOS + place).astype(jnp.int32)

    def to_patches(grid):
        shaped = grid.reshape(N_SLAB, CZ, N_ROW, CY, GX).transpose(0, 2, 1, 3, 4)
        return shaped.reshape(dev_count * NPOS, PT)

    def from_patches(rows_all):
        shaped = rows_all.reshape(N_SLAB, N_ROW, CZ, CY, GX).transpose(0, 2, 1, 3, 4)
        return shaped.reshape(NZ, NY, GX)

    for timestep in range(STEPS):
        sampled = to_patches(potential)[patch_of]
        outside = jnp.dot(transfer.T, sampled.T, precision=lax.Precision.HIGHEST, preferred_element_type=jnp.float32)
        voltage = hines_solve(voltage + outside, inverses, parents)
        membrane = conductance[:, None] * (voltage - outside)
        deposit = jnp.dot(transfer, membrane, precision=lax.Precision.HIGHEST, preferred_element_type=jnp.float32)
        summed = jax.ops.segment_sum(deposit.T, patch_of, num_segments=dev_count * NPOS)
        source = from_patches(summed)
        for repeat in range(SWEEPS):
            potential = relax_grid(potential, source)
    return voltage, potential
```

```python
import functools
import jax, jax.numpy as jnp
from jax import lax
from jax.experimental import pallas as pl
from jax.experimental.pallas import tpu as pltpu

from jax.sharding import PartitionSpec as P

STEPS = 2
SWEEPS = 4


screening = 0.25
coupling = 0.5


def padded_2(block, sides, width):
    for axis, dim in sides:
        count = lax.axis_size(axis)
        forward = [(i, i + 1) for i in range(count - 1)]
        backward = [(target, source) for source, target in forward]
        low = lax.ppermute(
            lax.slice_in_dim(block, block.shape[dim] - width, None, axis=dim), axis, forward
        )
        high = lax.ppermute(lax.slice_in_dim(block, 0, width, axis=dim), axis, backward)
        block = jnp.concatenate([low, block, high], axis=dim)
    return block


def hines_solve(rhs, inverses, parents):
    number = inverses.shape[0]
    width = inverses.shape[1]
    blocks = rhs.reshape(number, width, rhs.shape[1])
    solved = []
    for segment in range(number):
        right = blocks[segment]
        if segment > 0:
            above = jnp.zeros_like(right)
            for earlier in range(segment):
                above = above + jnp.where(
                    parents[segment - 1] == earlier, solved[earlier], jnp.zeros_like(right)
                )
            right = right + coupling * above
        solved.append(
            jnp.dot(
                inverses[segment],
                right,
                precision=lax.Precision.HIGHEST,
                preferred_element_type=jnp.float32,
            )
        )
    return jnp.concatenate(solved, axis=0)


def neighbours(field):
    padded = jnp.pad(field, 1)
    beside = padded[2:, 1:-1, 1:-1] + padded[:-2, 1:-1, 1:-1]
    beside = beside + padded[1:-1, 2:, 1:-1] + padded[1:-1, :-2, 1:-1]
    return beside + padded[1:-1, 1:-1, 2:] + padded[1:-1, 1:-1, :-2]


def peer_of(offset):
    slab = lax.axis_index("slab"); row = lax.axis_index("row")
    core = (slab + offset) % 2
    y = (slab // 2 + offset // 2) % 4
    x = (row + offset // 8) % 4
    z = (slab // 8 + offset // 32) % 4
    return z * 8 + y * 2 + core, x

def kernel(table, out, send_sem, recv_sem):
    slab = lax.axis_index("slab"); row = lax.axis_index("row")
    me = slab * 4 + row
    barrier = pltpu.get_barrier_semaphore()
    def greet(o, c):
        s, r = peer_of(o)
        pl.semaphore_signal(barrier, inc=1, device_id={"slab": s, "row": r})
        return c
    lax.fori_loop(1, 128, greet, 0)
    pl.semaphore_wait(barrier, 127)
    def send(o, c):
        s, r = peer_of(o)
        pltpu.make_async_remote_copy(
            src_ref=table.at[s * 4 + r], dst_ref=out.at[me], send_sem=send_sem, recv_sem=recv_sem,
            device_id={"slab": s, "row": r}).start()
        return c
    lax.fori_loop(1, 128, send, 0)
    out[me] = table[me]
    pltpu.make_async_copy(table.at[pl.ds(0, 127)], out.at[pl.ds(0, 127)], recv_sem).wait()
    pltpu.make_async_copy(table.at[pl.ds(0, 127)], table.at[pl.ds(0, 127)], send_sem).wait()

def a2a(table, cid):
    return pl.pallas_call(kernel, out_shape=jax.ShapeDtypeStruct(table.shape, table.dtype),
        in_specs=[pl.BlockSpec(memory_space=pltpu.VMEM)], out_specs=pl.BlockSpec(memory_space=pltpu.VMEM),
        scratch_shapes=[pltpu.SemaphoreType.DMA, pltpu.SemaphoreType.DMA],
        compiler_params=pltpu.CompilerParams(collective_id=cid, has_side_effects=True))(table)


def send_places(table):
    arrived = lax.all_to_all(table, ("slab", "row"), split_axis=0, concat_axis=0, tiled=True)
    return arrived


def send_currents(table):
    arrived = a2a(table, 0)
    return arrived


def send_potentials(table):
    arrived = a2a(table, 0)
    return arrived


def relax_grid(potential, source):
    depth_z = potential.shape[0]
    depth_y = potential.shape[1]
    stacked = jnp.stack([potential, source])
    extended = padded_2(stacked, (("slab", 1), ("row", 2)), SWEEPS)
    zplace = (
        lax.axis_index("slab") * depth_z
        - SWEEPS
        + jnp.arange(depth_z + 2 * SWEEPS, dtype=jnp.int32)
    )
    yplace = (
        lax.axis_index("row") * depth_y - SWEEPS + jnp.arange(depth_y + 2 * SWEEPS, dtype=jnp.int32)
    )
    zinside = (zplace >= 0) & (zplace < depth_z * lax.axis_size("slab"))
    yinside = (yplace >= 0) & (yplace < depth_y * lax.axis_size("row"))
    inside = zinside[:, None, None] & yinside[None, :, None]
    field = extended[0]
    feeding = extended[1]
    for repeat in range(SWEEPS):
        field = jnp.where(
            inside, (neighbours(field) + feeding) / (6.0 + screening), jnp.zeros_like(field)
        )
    result = field[SWEEPS:-SWEEPS, SWEEPS:-SWEEPS]
    return result


def shards(voltage, potential, transfer, conductance, inverses, parents, target, place):
    slabs = lax.axis_size("slab")
    lines = lax.axis_size("row")
    devices = slabs * lines
    local_cells = voltage.shape[1]
    capacity = max(2, 2 * local_cells // devices)
    patch_len = transfer.shape[0]
    positions = potential.size // patch_len
    owners = target[:, 0]
    one_hot = (owners[:, None] == jnp.arange(devices, dtype=jnp.int32)[None, :]).astype(jnp.int32)
    before = jnp.cumsum(one_hot, axis=0) - one_hot
    order_in = jnp.sum(before * one_hot, axis=1)
    slot_index = owners * capacity + order_in
    places = jnp.full((devices * capacity,), -1, jnp.int32).at[slot_index].set(place)
    arrived_places = send_places(places.reshape(devices, capacity)).reshape(devices * capacity)
    filled = arrived_places >= 0
    fetch_rows = jnp.where(filled, arrived_places, jnp.zeros_like(arrived_places))
    drop_rows = jnp.where(filled, arrived_places, jnp.full_like(arrived_places, positions))
    for timestep in range(STEPS):
        grid_rows = potential.reshape(positions, patch_len)
        picked = jnp.where(
            filled[:, None], grid_rows[fetch_rows], jnp.zeros((1, patch_len), jnp.float32)
        )
        returned = send_potentials(picked.reshape(devices, capacity, patch_len))
        sampled = returned.reshape(devices * capacity, patch_len)[slot_index]
        outside = lax.dot_general(
            transfer,
            sampled,
            (((0,), (1,)), ((), ())),
            precision=lax.Precision.HIGHEST,
            preferred_element_type=jnp.float32,
        )
        voltage = hines_solve(voltage + outside, inverses, parents)
        membrane = conductance[:, None] * (voltage - outside)
        deposit = jnp.dot(
            transfer, membrane, precision=lax.Precision.HIGHEST, preferred_element_type=jnp.float32
        )
        outgoing = (
            jnp.zeros((devices * capacity, patch_len), jnp.float32).at[slot_index].set(deposit.T)
        )
        arrived = send_currents(outgoing.reshape(devices, capacity, patch_len))
        summed = (
            jnp.zeros((positions, patch_len), jnp.float32)
            .at[drop_rows]
            .add(arrived.reshape(devices * capacity, patch_len), mode="drop")
        )
        source = summed.reshape(potential.shape)
        potential = relax_grid(potential, source)
    return (voltage, potential)


def solution(mesh):
    return jax.shard_map(
        shards,
        mesh=mesh,
        in_specs=(
            P(None, ("slab", "row")),
            P("slab", "row", None),
            P(),
            P(),
            P(),
            P(),
            P(("slab", "row"), None),
            P(("slab", "row")),
        ),
        out_specs=(P(None, ("slab", "row")), P("slab", "row", None)),
        check_vma=False,
    )
```

```python
import jax
import jax.numpy as jnp
from jax import lax
from jax.experimental import pallas as pl
from jax.experimental.pallas import tpu as pltpu
from jax.sharding import PartitionSpec as P

SWEEPS = 4
CAP = 12
SLOT = 16
DEVS = 128
WALK = 37
scale = 1.0 / 6.25
coupling = 0.5
F32 = jnp.float32
BF16 = jnp.bfloat16
ROWS = (((1,), (0,)), ((), ()))
BOTH = (((1,), (1,)), ((), ()))
DIRS = tuple((dz, dy) for dz in (-1, 0, 1) for dy in (-1, 0, 1) if (dz, dy) != (0, 0))


def split(value):
    high = value.astype(BF16)
    return high, (value - high.astype(F32)).astype(BF16)


def dot1(a, b, dims=ROWS):
    return lax.dot_general(a, b, dims, preferred_element_type=F32)


def dot3(a, b, dims=ROWS):
    ah, al = split(a)
    bh, bl = split(b)
    return dot1(ah, bh, dims) + (dot1(ah, bl, dims) + dot1(al, bh, dims))


def kernel(
    volt, pot, trans, cond, inv, par, tgt, plc, volt_out, pot_out,
    ohc, ohp, oht, gmat, amat, ymat, coef, pt, zmat, lt, grid, sc0, se0, cnt,
    snd1, rcv1, snd2, rcv2, snd3, rcv3, snd4, rcv4,
    f0, f1, r1, r2, xa, xb,
    a2a_send, a2a_recv, halo_send, halo_recv,
):
    slab = lax.axis_index("slab")
    row = lax.axis_index("row")
    me = slab * 4 + row
    depth = pot.shape[0]
    lines = pot.shape[1]
    cells = volt.shape[1]
    half = depth * lines

    def walk(step):
        d = lax.rem(me + step * WALK, DEVS)
        return d, {"slab": lax.div(d, 4), "row": lax.rem(d, 4)}

    barrier = pltpu.get_barrier_semaphore()

    def greet(step, carry):
        _, where = walk(step)
        pl.semaphore_signal(barrier, inc=1, device_id=where)
        return carry

    for ref in (f0, f1, r1, r2):
        @pl.when(slab == 0)
        def _():
            ref[0:SWEEPS] = jnp.zeros((SWEEPS,) + ref.shape[1:], F32)

        @pl.when(slab == 31)
        def _():
            ref[depth + SWEEPS:] = jnp.zeros((SWEEPS,) + ref.shape[1:], F32)

        @pl.when(row == 0)
        def _():
            ref[:, 0:8] = jnp.zeros((ref.shape[0], 8, ref.shape[2]), F32)

        @pl.when(row == 3)
        def _():
            ref[:, lines + 8:] = jnp.zeros((ref.shape[0], 8, ref.shape[2]), F32)

    lax.fori_loop(1, DEVS, greet, 0)

    f0[SWEEPS:SWEEPS + depth, 8:8 + lines] = pot[...]

    owner = tgt[...]
    place = plc[...]
    own = (owner == lax.broadcasted_iota(jnp.int32, (DEVS, cells), 0)).astype(F32)
    ownb = own.astype(BF16)
    earlier = (
        lax.broadcasted_iota(jnp.int32, (cells, cells), 0)
        < lax.broadcasted_iota(jnp.int32, (cells, cells), 1)
    ).astype(F32).astype(BF16)
    before = dot1(ownb, earlier)
    order = jnp.sum(before * own, axis=0, keepdims=True)
    for k in range(CAP):
        ohc[k * DEVS:(k + 1) * DEVS, :] = (own * (order == float(k)).astype(F32)).astype(BF16)
    spot = lax.rem(place, 2) * half + lax.div(place, 2) + 1
    ranks = lax.broadcasted_iota(jnp.int32, (DEVS, cells), 0).astype(F32)
    here = (ranks == order).astype(F32)
    upper = lax.div(spot, 16).astype(F32)
    lower = lax.rem(spot, 16).astype(F32)
    table = 16.0 * dot1(ownb, (here * upper).astype(BF16), BOTH) + dot1(
        ownb, (here * lower).astype(BF16), BOTH
    )
    snd1[pl.ds(CAP, DEVS, stride=SLOT), :] = table

    for k in range(8):
        unit = (
            lax.broadcasted_iota(jnp.int32, (64, 512), 0) + 64 * k
            == lax.broadcasted_iota(jnp.int32, (64, 512), 1)
        ).astype(F32)
        for earlier_block in range(k):
            above = amat[64 * earlier_block:64 * (earlier_block + 1), :]
            unit = unit + jnp.where(
                par[0:1, k - 1:k] == earlier_block, coupling * above, jnp.zeros_like(above)
            )
        amat[64 * k:64 * (k + 1), :] = lax.dot_general(
            inv[k], unit, ROWS, precision=lax.Precision.HIGHEST, preferred_element_type=F32
        )
    weighted = trans[...] * cond[...]
    back = dot3(weighted, amat[...])
    back2 = dot3(back, amat[...])
    cmat = dot3(back - weighted, trans[...], BOTH)
    emat = dot3(back2, trans[...], BOTH)
    coef[0:128, :] = cmat
    coef[128:256, :] = emat

    def to_slots(hot, parts, snd):
        for group in range(CAP // 4):
            got = dot1(hot[group * 512:(group + 1) * 512, :], parts[...])
            got = got[:, 0:128] + got[:, 128:256]
            for k in range(4):
                snd[pl.ds(group * 4 + k, DEVS, stride=SLOT), :] = got[k * 128:(k + 1) * 128]

    def fill(weights, snd):
        made = dot3(weights, volt[...])
        high, low = split(jnp.transpose(made))
        pt[:, 0:128] = high
        pt[:, 128:256] = low
        to_slots(ohc, pt, snd)

    def send_all(number, snd, rcv, rows):
        def send(step, carry):
            d, where = walk(step)
            pltpu.make_async_remote_copy(
                src_ref=snd.at[pl.ds(pl.multiple_of(d * SLOT, SLOT), rows)],
                dst_ref=rcv.at[pl.ds(pl.multiple_of(me * SLOT, SLOT), rows)],
                send_sem=a2a_send.at[number],
                recv_sem=a2a_recv.at[number],
                device_id=where,
            ).start()
            return carry

        lax.fori_loop(1, DEVS, send, 0)
        mine = pl.ds(pl.multiple_of(me * SLOT, SLOT), SLOT)
        rcv[mine, :] = snd[mine, :]

    def arrived(number, rcv, rows):
        total = pl.ds(0, (DEVS - 1) * rows)
        pltpu.make_async_copy(rcv.at[total], rcv.at[total], a2a_recv.at[number]).wait()

    def departed(number, snd, rows):
        total = pl.ds(0, (DEVS - 1) * rows)
        pltpu.make_async_copy(snd.at[total], snd.at[total], a2a_send.at[number]).wait()

    def span(shift, first, count, width, low, wide):
        if shift == 0:
            return pl.ds(first, count), pl.ds(first, count)
        if shift < 0:
            return pl.ds(first, wide), pl.ds(first + count, wide)
        return pl.ds(first + count - wide, wide), pl.ds(first - wide, wide)

    def halo(number, ref, planes, act):
        for spot_of, (dz, dy) in enumerate(DIRS):
            zs, zd = span(dz, SWEEPS, depth, None, None, planes)
            ys, yd = span(dy, 8, lines, None, None, 8)
            copy = pltpu.make_async_remote_copy(
                src_ref=ref.at[zs, ys],
                dst_ref=ref.at[zd, yd],
                send_sem=halo_send.at[number * 8 + spot_of],
                recv_sem=halo_recv.at[number * 8 + spot_of],
                device_id={"slab": slab + dz, "row": row + dy},
            )
            to = (slab + dz >= 0) & (slab + dz <= 31) & (row + dy >= 0) & (row + dy <= 3)
            came = (slab - dz >= 0) & (slab - dz <= 31) & (row - dy >= 0) & (row - dy <= 3)
            if act == "start":
                @pl.when(to)
                def _():
                    copy.start()
            elif act == "recv":
                @pl.when(came)
                def _():
                    copy.wait_recv()
            else:
                @pl.when(to)
                def _():
                    copy.wait_send()

    fill(back, snd1)

    pl.semaphore_wait(barrier, DEVS - 1)
    send_all(0, snd1, rcv1, CAP + 1)
    halo(0, f0, SWEEPS, "start")
    fill(back2, snd2)

    grid[0:half, :] = pot[:, :, 0:128].reshape(half, 128)
    grid[half:, :] = pot[:, :, 128:256].reshape(half, 128)
    for q in range(4):
        rows_of = pl.ds(q * 512, 512)
        part = grid[rows_of, :]
        sc0[rows_of, :] = dot3(part, coef[0:128, :], BOTH)
        se0[rows_of, :] = dot3(part, coef[128:256, :], BOTH)
    first = dot3(amat[...], trans[...], BOTH)
    second = dot3(amat[...], first)
    ymat[...] = dot3(amat[...], volt[...])
    ymat[...] = dot3(amat[...], ymat[...])

    def rows_in(rcv):
        for k in range(CAP):
            high, low = split(rcv[pl.ds(k, DEVS, stride=SLOT), :])
            zmat[k * DEVS:(k + 1) * DEVS, 0:128] = high
            zmat[k * DEVS:(k + 1) * DEVS, 128:256] = low

    def place_rows(ref, q, value):
        z = SWEEPS + (q % 2) * 4
        x = (q // 2) * 128
        ref[z:z + 4, 8:8 + lines, x:x + 128] = value.reshape(4, lines, 128)

    arrived(0, rcv1, CAP + 1)
    asked = rcv1[pl.ds(CAP, DEVS, stride=SLOT), :] - 1.0
    asked_t = jnp.transpose(asked)
    rows_in(rcv1)
    ones = jnp.ones((128, 128), BF16)
    for q in range(4):
        rows_of = pl.ds(q * 512, 512)
        spots = (lax.broadcasted_iota(jnp.int32, (512, 128), 0) + q * 512).astype(F32)
        many = jnp.zeros((512, 128), F32)
        for k in range(CAP):
            hit = (asked_t[k:k + 1, :] == spots).astype(F32)
            many = many + hit
            ohp[rows_of, k * 128:(k + 1) * 128] = hit.astype(BF16)
        count = dot1(many.astype(BF16), ones)
        cnt[rows_of, :] = count
        got = dot1(ohp[rows_of, :], zmat[...])
        place_rows(r1, q, got[:, 0:128] + got[:, 128:256] + count * sc0[rows_of, :])
    halo(1, r1, 3, "start")
    send_all(1, snd2, rcv2, CAP)
    for q in range(4):
        spots = (lax.broadcasted_iota(jnp.int32, (128, 512), 1) + q * 512).astype(F32)
        for k in range(CAP):
            hit = (asked[:, k:k + 1] == spots).astype(F32)
            oht[k * 128:(k + 1) * 128, q * 512:(q + 1) * 512] = hit.astype(BF16)

    def gather(snd):
        high, low = split(grid[...])
        gmat[:, 0:128] = high
        gmat[:, 128:256] = low
        to_slots(oht, gmat, snd)

    gather(snd3)
    send_all(2, snd3, rcv3, CAP)

    rowsy = lax.broadcasted_iota(jnp.int32, (lines + 16, 256), 0) + (row * lines - 8)
    inside = ((rowsy >= 0) & (rowsy < 4 * lines)).astype(F32) * scale
    lanes = lax.broadcasted_iota(jnp.int32, (lines + 16, 256), 1)

    def sweep(number, src, feed, dst, last):
        def plane(z, carry):
            mid = src[z]
            total = src[z - 1] + src[z + 1] + feed[z]
            total = total + pltpu.roll(mid, 1, 0) + pltpu.roll(mid, lines + 15, 0)
            total = total + jnp.where(lanes == 0, 0.0, pltpu.roll(mid, 1, 1))
            total = total + jnp.where(lanes == 255, 0.0, pltpu.roll(mid, 255, 1))
            at = slab * depth - SWEEPS + z
            held = ((at >= 0) & (at < 32 * depth)).astype(F32)
            value = total * (inside * held)
            if last == "grid":
                dst[z, 8:8 + lines] = value[8:8 + lines]
            elif last == "out":
                dst[z - SWEEPS] = value[8:8 + lines]
            else:
                dst[z] = value
            return carry

        lax.fori_loop(number, depth + 2 * SWEEPS - number, plane, 0)

    halo(0, f0, SWEEPS, "recv")
    halo(1, r1, 3, "recv")
    sweep(1, f0, r1, xa, "")
    sweep(2, xa, r1, xb, "")
    sweep(3, xb, r1, xa, "")
    sweep(4, xa, r1, f1, "grid")
    halo(2, f1, SWEEPS, "start")
    for z in range(depth):
        grid[z * lines:(z + 1) * lines, :] = f1[SWEEPS + z, 8:8 + lines, 0:128]
        grid[half + z * lines:half + (z + 1) * lines, :] = f1[SWEEPS + z, 8:8 + lines, 128:256]
    gather(snd4)
    send_all(3, snd4, rcv4, CAP)

    arrived(1, rcv2, CAP)
    rows_in(rcv2)
    for q in range(4):
        rows_of = pl.ds(q * 512, 512)
        got = dot1(ohp[rows_of, :], zmat[...])
        more = se0[rows_of, :] + dot3(grid[rows_of, :], coef[0:128, :], BOTH)
        place_rows(r2, q, got[:, 0:128] + got[:, 128:256] + cnt[rows_of, :] * more)
    halo(3, r2, 3, "start")

    def bring(number, rcv, weights):
        arrived(number, rcv, CAP)
        for k in range(CAP):
            high, low = split(jnp.transpose(rcv[pl.ds(k, DEVS, stride=SLOT), :]))
            lt[0:128, k * 128:(k + 1) * 128] = high
            lt[128:256, k * 128:(k + 1) * 128] = low
        got = dot1(lt[...], ohc[...])
        return dot3(weights, got[0:128, :] + got[128:256, :])

    ymat[...] = ymat[...] + bring(2, rcv3, second)
    halo(2, f1, SWEEPS, "recv")
    halo(3, r2, 3, "recv")
    sweep(1, f1, r2, xa, "")
    sweep(2, xa, r2, xb, "")
    sweep(3, xb, r2, xa, "")
    sweep(4, xa, r2, pot_out, "out")
    volt_out[...] = ymat[...] + bring(3, rcv4, first)
    departed(0, snd1, CAP + 1)
    departed(1, snd2, CAP)
    departed(2, snd3, CAP)
    departed(3, snd4, CAP)
    halo(0, f0, SWEEPS, "sent")
    halo(1, r1, 3, "sent")
    halo(2, f1, SWEEPS, "sent")
    halo(3, r2, 3, "sent")


def shards(voltage, potential, transfer, conductance, inverses, parents, target, place):
    cells = voltage.shape[1]
    depth, lines, wide = potential.shape
    tall = (depth + 2 * SWEEPS, lines + 16, wide)
    vmem = pl.BlockSpec(memory_space=pltpu.VMEM)
    block = pltpu.VMEM((DEVS * SLOT, 128), F32)
    return pl.pallas_call(
        kernel,
        out_shape=(
            jax.ShapeDtypeStruct(voltage.shape, F32),
            jax.ShapeDtypeStruct(potential.shape, F32),
        ),
        in_specs=[vmem] * 8,
        out_specs=(vmem, vmem),
        scratch_shapes=[
            pltpu.VMEM((CAP * DEVS, cells), BF16),
            pltpu.VMEM((depth * lines * 2, CAP * DEVS), BF16),
            pltpu.VMEM((CAP * DEVS, depth * lines * 2), BF16),
            pltpu.VMEM((depth * lines * 2, 256), BF16),
            pltpu.VMEM((512, 512), F32),
            pltpu.VMEM((512, cells), F32),
            pltpu.VMEM((256, 128), F32),
            pltpu.VMEM((cells, 256), BF16),
            pltpu.VMEM((CAP * DEVS, 256), BF16),
            pltpu.VMEM((256, CAP * DEVS), BF16),
            pltpu.VMEM((depth * lines * 2, 128), F32),
            pltpu.VMEM((depth * lines * 2, 128), F32),
            pltpu.VMEM((depth * lines * 2, 128), F32),
            pltpu.VMEM((depth * lines * 2, 128), F32),
        ]
        + [block] * 8
        + [pltpu.VMEM(tall, F32)] * 6
        + [
            pltpu.SemaphoreType.DMA((4,)),
            pltpu.SemaphoreType.DMA((4,)),
            pltpu.SemaphoreType.DMA((32,)),
            pltpu.SemaphoreType.DMA((32,)),
        ],
        compiler_params=pltpu.CompilerParams(
            collective_id=0, has_side_effects=True, vmem_limit_bytes=60 * 1024 * 1024
        ),
    )(
        voltage, potential, transfer, conductance.reshape(1, -1), inverses, parents.reshape(1, -1),
        target.reshape(1, -1), place.reshape(1, -1),
    )


def solution(mesh):
    return jax.shard_map(
        shards,
        mesh=mesh,
        in_specs=(
            P(None, ("slab", "row")),
            P("slab", "row", None),
            P(),
            P(),
            P(),
            P(),
            P(("slab", "row"), None),
            P(("slab", "row")),
        ),
        out_specs=(P(None, ("slab", "row")), P("slab", "row", None)),
        check_vma=False,
    )
```

```python
import jax
import jax.numpy as jnp
from jax import lax
from jax.experimental import pallas as pl
from jax.experimental.pallas import tpu as pltpu
from jax.sharding import PartitionSpec as P

SWEEPS = 4
CAP = 12
SLOT = 16
DEVS = 128
WALK = 37
scale = 1.0 / 6.25
coupling = 0.5
F32 = jnp.float32
BF16 = jnp.bfloat16
ROWS = (((1,), (0,)), ((), ()))
BOTH = (((1,), (1,)), ((), ()))
DIRS = ((-1, 0), (1, 0), (0, -1), (0, 1))


def split(value):
    high = value.astype(BF16)
    return high, (value - high.astype(F32)).astype(BF16)


def dot1(a, b, dims=ROWS):
    return lax.dot_general(a, b, dims, preferred_element_type=F32)


def dot3(a, b, dims=ROWS):
    ah, al = split(a)
    bh, bl = split(b)
    return dot1(ah, bh, dims) + (dot1(ah, bl, dims) + dot1(al, bh, dims))


def kernel(
    volt, pot, trans, cond, inv, par, tgt, plc, volt_out, pot_out,
    ohc, ohp, oht, gmat, amat, ymat, coef, pt, zmat, lt, grid, sc0, se0, cnt,
    snd1, rcv1, snd2, rcv2, snd3, rcv3, snd4, rcv4,
    field, feed,
    a2a_send, a2a_recv, halo_send, halo_recv,
):
    slab = lax.axis_index("slab")
    row = lax.axis_index("row")
    me = slab * 4 + row
    depth = pot.shape[0]
    lines = pot.shape[1]
    cells = volt.shape[1]
    half = depth * lines

    def walk(step):
        d = lax.rem(me + step * WALK, DEVS)
        return d, {"slab": lax.div(d, 4), "row": lax.rem(d, 4)}

    barrier = pltpu.get_barrier_semaphore()

    def greet(step, carry):
        _, where = walk(step)
        pl.semaphore_signal(barrier, inc=1, device_id=where)
        return carry

    edge = (field.shape[0], 1) + field.shape[2:]
    side = (field.shape[0], depth + 2, 8, field.shape[3])

    @pl.when(slab == 0)
    def _():
        field[:, 0:1] = jnp.zeros(edge, F32)

    @pl.when(slab == 31)
    def _():
        field[:, depth + 1:] = jnp.zeros(edge, F32)

    @pl.when(row == 0)
    def _():
        field[:, :, 0:8] = jnp.zeros(side, F32)

    @pl.when(row == 3)
    def _():
        field[:, :, lines + 8:] = jnp.zeros(side, F32)

    lax.fori_loop(1, DEVS, greet, 0)

    field[0, 1:1 + depth, 8:8 + lines] = pot[...]

    owner = tgt[...]
    place = plc[...]
    own = (owner == lax.broadcasted_iota(jnp.int32, (DEVS, cells), 0)).astype(F32)
    ownb = own.astype(BF16)
    earlier = (
        lax.broadcasted_iota(jnp.int32, (cells, cells), 0)
        < lax.broadcasted_iota(jnp.int32, (cells, cells), 1)
    ).astype(F32).astype(BF16)
    before = dot1(ownb, earlier)
    order = jnp.sum(before * own, axis=0, keepdims=True)
    for k in range(CAP):
        ohc[k * DEVS:(k + 1) * DEVS, :] = (own * (order == float(k)).astype(F32)).astype(BF16)
    spot = lax.rem(place, 2) * half + lax.div(place, 2) + 1
    ranks = lax.broadcasted_iota(jnp.int32, (DEVS, cells), 0).astype(F32)
    here = (ranks == order).astype(F32)
    upper = lax.div(spot, 16).astype(F32)
    lower = lax.rem(spot, 16).astype(F32)
    table = 16.0 * dot1(ownb, (here * upper).astype(BF16), BOTH) + dot1(
        ownb, (here * lower).astype(BF16), BOTH
    )
    snd1[pl.ds(CAP, DEVS, stride=SLOT), :] = table

    for k in range(8):
        unit = (
            lax.broadcasted_iota(jnp.int32, (64, 512), 0) + 64 * k
            == lax.broadcasted_iota(jnp.int32, (64, 512), 1)
        ).astype(F32)
        for earlier_block in range(k):
            above = amat[64 * earlier_block:64 * (earlier_block + 1), :]
            unit = unit + jnp.where(
                par[0:1, k - 1:k] == earlier_block, coupling * above, jnp.zeros_like(above)
            )
        amat[64 * k:64 * (k + 1), :] = lax.dot_general(
            inv[k], unit, ROWS, precision=lax.Precision.HIGHEST, preferred_element_type=F32
        )
    weighted = trans[...] * cond[...]
    back = dot3(weighted, amat[...])
    back2 = dot3(back, amat[...])
    cmat = dot3(back - weighted, trans[...], BOTH)
    emat = dot3(back2, trans[...], BOTH)
    coef[0:128, :] = cmat
    coef[128:256, :] = emat

    def to_slots(hot, parts, snd):
        for group in range(CAP // 4):
            got = dot1(hot[group * 512:(group + 1) * 512, :], parts[...])
            got = got[:, 0:128] + got[:, 128:256]
            for k in range(4):
                snd[pl.ds(group * 4 + k, DEVS, stride=SLOT), :] = got[k * 128:(k + 1) * 128]

    def fill(weights, snd):
        made = dot3(weights, volt[...])
        high, low = split(jnp.transpose(made))
        pt[:, 0:128] = high
        pt[:, 128:256] = low
        to_slots(ohc, pt, snd)

    def send_part(number, snd, rcv, rows, first, last):
        def send(step, carry):
            d, where = walk(step)
            pltpu.make_async_remote_copy(
                src_ref=snd.at[pl.ds(pl.multiple_of(d * SLOT, SLOT), rows)],
                dst_ref=rcv.at[pl.ds(pl.multiple_of(me * SLOT, SLOT), rows)],
                send_sem=a2a_send.at[number],
                recv_sem=a2a_recv.at[number],
                device_id=where,
            ).start()
            return carry

        lax.fori_loop(max(first * DEVS // 4, 1), last * DEVS // 4, send, 0)
        if last == 4:
            mine = pl.ds(pl.multiple_of(me * SLOT, SLOT), SLOT)
            rcv[mine, :] = snd[mine, :]

    def arrived(number, rcv, rows):
        total = pl.ds(0, (DEVS - 1) * rows)
        pltpu.make_async_copy(rcv.at[total], rcv.at[total], a2a_recv.at[number]).wait()

    def departed(number, snd, rows):
        total = pl.ds(0, (DEVS - 1) * rows)
        pltpu.make_async_copy(snd.at[total], snd.at[total], a2a_send.at[number]).wait()

    def halo(number, act):
        ref = field.at[number]
        for at, (dz, dy) in enumerate(DIRS):
            inner_z = pl.ds(1, depth)
            inner_y = pl.ds(8, lines)
            if dz:
                src = ref.at[pl.ds(1 if dz < 0 else depth, 1), inner_y]
                dst = ref.at[pl.ds(depth + 1 if dz < 0 else 0, 1), inner_y]
            else:
                src = ref.at[inner_z, pl.ds(8 if dy < 0 else lines, 8)]
                dst = ref.at[inner_z, pl.ds(lines + 8 if dy < 0 else 0, 8)]
            copy = pltpu.make_async_remote_copy(
                src_ref=src,
                dst_ref=dst,
                send_sem=halo_send.at[number * 4 + at],
                recv_sem=halo_recv.at[number * 4 + at],
                device_id={"slab": slab + dz, "row": row + dy},
            )
            to = (slab + dz >= 0) & (slab + dz <= 31) & (row + dy >= 0) & (row + dy <= 3)
            came = (slab - dz >= 0) & (slab - dz <= 31) & (row - dy >= 0) & (row - dy <= 3)
            if act == "start":
                pl.when(to)(copy.start)
            elif act == "recv":
                pl.when(came)(copy.wait_recv)
            else:
                pl.when(to)(copy.wait_send)

    fill(back, snd1)

    pl.semaphore_wait(barrier, DEVS - 1)
    halo(0, "start")
    send_part(0, snd1, rcv1, CAP + 1, 0, 4)
    fill(back2, snd2)
    send_part(1, snd2, rcv2, CAP, 0, 2)

    grid[0:half, :] = pot[:, :, 0:128].reshape(half, 128)
    grid[half:, :] = pot[:, :, 128:256].reshape(half, 128)
    for q in range(4):
        rows_of = pl.ds(q * 512, 512)
        part = grid[rows_of, :]
        sc0[rows_of, :] = dot3(part, coef[0:128, :], BOTH)
        se0[rows_of, :] = dot3(part, coef[128:256, :], BOTH)
    first = dot3(amat[...], trans[...], BOTH)
    second = dot3(amat[...], first)
    ymat[...] = dot3(amat[...], volt[...])
    ymat[...] = dot3(amat[...], ymat[...])

    def rows_in(rcv):
        for k in range(CAP):
            high, low = split(rcv[pl.ds(k, DEVS, stride=SLOT), :])
            zmat[k * DEVS:(k + 1) * DEVS, 0:128] = high
            zmat[k * DEVS:(k + 1) * DEVS, 128:256] = low

    def place_rows(number, q, value):
        z = (q % 2) * 4
        x = (q // 2) * 128
        feed[number, z:z + 4, :, x:x + 128] = value.reshape(4, lines, 128)

    arrived(0, rcv1, CAP + 1)
    asked = rcv1[pl.ds(CAP, DEVS, stride=SLOT), :] - 1.0
    asked_t = jnp.transpose(asked)
    rows_in(rcv1)
    ones = jnp.ones((128, 128), BF16)
    for q in range(4):
        rows_of = pl.ds(q * 512, 512)
        spots = (lax.broadcasted_iota(jnp.int32, (512, 128), 0) + q * 512).astype(F32)
        many = jnp.zeros((512, 128), F32)
        for k in range(CAP):
            hit = (asked_t[k:k + 1, :] == spots).astype(F32)
            many = many + hit
            ohp[rows_of, k * 128:(k + 1) * 128] = hit.astype(BF16)
        count = dot1(many.astype(BF16), ones)
        cnt[rows_of, :] = count
        got = dot1(ohp[rows_of, :], zmat[...])
        place_rows(0, q, got[:, 0:128] + got[:, 128:256] + count * sc0[rows_of, :])
    def table_of_asked():
        for q in range(4):
            spots = (lax.broadcasted_iota(jnp.int32, (128, 512), 1) + q * 512).astype(F32)
            for k in range(CAP):
                hit = (asked[:, k:k + 1] == spots).astype(F32)
                oht[k * 128:(k + 1) * 128, q * 512:(q + 1) * 512] = hit.astype(BF16)

    def gather(snd):
        high, low = split(grid[...])
        gmat[:, 0:128] = high
        gmat[:, 128:256] = low
        to_slots(oht, gmat, snd)

    lane = lax.broadcasted_iota(jnp.int32, (8, 128), 1)
    line = lax.broadcasted_iota(jnp.int32, (8, 128), 0)
    zero = jnp.zeros((8, 128), F32)
    tiles = lines // 8

    def sweep(number):
        src = field.at[number]
        last = number + 1 == 2 * SWEEPS

        def tile(at_z, t, h):
            return src[at_z, 8 * t + 8:8 * t + 16, 128 * h:128 * h + 128]

        def strip(z, which):
            for t in which:
                left, right = tile(z, t, 0), tile(z, t, 1)
                before_x = (jnp.where(lane == 127, zero, left), jnp.where(lane == 127, left, right))
                after_x = (jnp.where(lane == 0, right, left), jnp.where(lane == 0, zero, right))
                for h, mid in enumerate((left, right)):
                    x = slice(128 * h, 128 * h + 128)
                    total = tile(z - 1, t, h) + tile(z + 1, t, h)
                    total = total + feed[number // SWEEPS, z - 1, 8 * t:8 * t + 8, x]
                    total = total + (
                        pltpu.roll(jnp.where(line == 7, tile(z, t - 1, h), mid), 1, 0)
                        + pltpu.roll(jnp.where(line == 0, tile(z, t + 1, h), mid), 7, 0)
                    )
                    total = total + (
                        pltpu.roll(before_x[h], 1, 1) + pltpu.roll(after_x[h], 127, 1)
                    )
                    if last:
                        pot_out[z - 1, 8 * t:8 * t + 8, x] = total * scale
                    else:
                        field[number + 1, z, 8 * t + 8:8 * t + 16, x] = total * scale

        def over(first, count, step, which):
            def body(i, carry):
                strip(first + i * step, which)
                return carry

            lax.fori_loop(0, count, body, 0)

        halo(number, "recv")
        if last:
            over(1, depth, 1, range(tiles))
        else:
            over(1, 2, depth - 1, range(tiles))
            over(2, depth - 2, 1, (0, tiles - 1))
            halo(number + 1, "start")
            over(2, depth - 2, 1, range(1, tiles - 1))

    def bring(number, rcv, weights):
        arrived(number, rcv, CAP)
        for k in range(CAP):
            high, low = split(jnp.transpose(rcv[pl.ds(k, DEVS, stride=SLOT), :]))
            lt[0:128, k * 128:(k + 1) * 128] = high
            lt[128:256, k * 128:(k + 1) * 128] = low
        got = dot1(lt[...], ohc[...])
        return dot3(weights, got[0:128, :] + got[128:256, :])

    sweep(0)
    send_part(1, snd2, rcv2, CAP, 2, 3)
    table_of_asked()
    sweep(1)
    send_part(1, snd2, rcv2, CAP, 3, 4)
    gather(snd3)
    sweep(2)
    send_part(2, snd3, rcv3, CAP, 0, 1)
    sweep(3)
    send_part(2, snd3, rcv3, CAP, 1, 3)
    for z in range(depth):
        now = field[SWEEPS, 1 + z, 8:8 + lines, :]
        grid[z * lines:(z + 1) * lines, :] = now[:, 0:128]
        grid[half + z * lines:half + (z + 1) * lines, :] = now[:, 128:256]
    for q in range(4):
        rows_of = pl.ds(q * 512, 512)
        se0[rows_of, :] = cnt[rows_of, :] * (
            se0[rows_of, :] + dot3(grid[rows_of, :], coef[0:128, :], BOTH)
        )
    arrived(1, rcv2, CAP)
    rows_in(rcv2)
    for q in range(4):
        rows_of = pl.ds(q * 512, 512)
        got = dot1(ohp[rows_of, :], zmat[...])
        place_rows(1, q, got[:, 0:128] + got[:, 128:256] + se0[rows_of, :])
    sweep(4)
    send_part(2, snd3, rcv3, CAP, 3, 4)
    gather(snd4)
    send_part(3, snd4, rcv4, CAP, 0, 1)
    sweep(5)
    send_part(3, snd4, rcv4, CAP, 1, 2)
    sweep(6)
    send_part(3, snd4, rcv4, CAP, 2, 4)
    sweep(7)
    ymat[...] = ymat[...] + bring(2, rcv3, second)
    volt_out[...] = ymat[...] + bring(3, rcv4, first)
    departed(0, snd1, CAP + 1)
    departed(1, snd2, CAP)
    departed(2, snd3, CAP)
    departed(3, snd4, CAP)
    for number in range(2 * SWEEPS):
        halo(number, "sent")


def shards(voltage, potential, transfer, conductance, inverses, parents, target, place):
    cells = voltage.shape[1]
    depth, lines, wide = potential.shape
    tall = (2 * SWEEPS, depth + 2, lines + 16, wide)
    vmem = pl.BlockSpec(memory_space=pltpu.VMEM)
    block = pltpu.VMEM((DEVS * SLOT, 128), F32)
    return pl.pallas_call(
        kernel,
        out_shape=(
            jax.ShapeDtypeStruct(voltage.shape, F32),
            jax.ShapeDtypeStruct(potential.shape, F32),
        ),
        in_specs=[vmem] * 8,
        out_specs=(vmem, vmem),
        scratch_shapes=[
            pltpu.VMEM((CAP * DEVS, cells), BF16),
            pltpu.VMEM((depth * lines * 2, CAP * DEVS), BF16),
            pltpu.VMEM((CAP * DEVS, depth * lines * 2), BF16),
            pltpu.VMEM((depth * lines * 2, 256), BF16),
            pltpu.VMEM((512, 512), F32),
            pltpu.VMEM((512, cells), F32),
            pltpu.VMEM((256, 128), F32),
            pltpu.VMEM((cells, 256), BF16),
            pltpu.VMEM((CAP * DEVS, 256), BF16),
            pltpu.VMEM((256, CAP * DEVS), BF16),
            pltpu.VMEM((depth * lines * 2, 128), F32),
            pltpu.VMEM((depth * lines * 2, 128), F32),
            pltpu.VMEM((depth * lines * 2, 128), F32),
            pltpu.VMEM((depth * lines * 2, 128), F32),
        ]
        + [block] * 8
        + [pltpu.VMEM(tall, F32), pltpu.VMEM((2, depth, lines, wide), F32)]
        + [
            pltpu.SemaphoreType.DMA((4,)),
            pltpu.SemaphoreType.DMA((4,)),
            pltpu.SemaphoreType.DMA((32,)),
            pltpu.SemaphoreType.DMA((32,)),
        ],
        compiler_params=pltpu.CompilerParams(
            collective_id=0, has_side_effects=True, vmem_limit_bytes=60 * 1024 * 1024
        ),
    )(
        voltage, potential, transfer, conductance.reshape(1, -1), inverses, parents.reshape(1, -1),
        target.reshape(1, -1), place.reshape(1, -1),
    )


def solution(mesh):
    return jax.shard_map(
        shards,
        mesh=mesh,
        in_specs=(
            P(None, ("slab", "row")),
            P("slab", "row", None),
            P(),
            P(),
            P(),
            P(),
            P(("slab", "row"), None),
            P(("slab", "row")),
        ),
        out_specs=(P(None, ("slab", "row")), P("slab", "row", None)),
        check_vma=False,
    )
```

```python
import jax
import jax.numpy as jnp
from jax import lax
from jax.experimental import pallas as pl
from jax.experimental.pallas import tpu as pltpu
from jax.sharding import PartitionSpec as P

SWEEPS = 4
CAP = 12
SLOT = 16
DEVS = 128
WALK = 37
scale = 1.0 / 6.25
coupling = 0.5
F32 = jnp.float32
BF16 = jnp.bfloat16
ROWS = (((1,), (0,)), ((), ()))
BOTH = (((1,), (1,)), ((), ()))
DIRS = ((-1, 0), (1, 0), (0, -1), (0, 1))


def split(value):
    high = value.astype(BF16)
    return high, (value - high.astype(F32)).astype(BF16)


def dot1(a, b, dims=ROWS):
    return lax.dot_general(a, b, dims, preferred_element_type=F32)


def dot3(a, b, dims=ROWS):
    ah, al = split(a)
    bh, bl = split(b)
    return dot1(ah, bh, dims) + (dot1(ah, bl, dims) + dot1(al, bh, dims))


def kernel(
    volt, pot, trans, cond, inv, par, tgt, plc, volt_out, pot_out, first_out, seen_out,
    ohc, ohp, oht, gmat, amat, ymat, coef, pt, zmat, lt, grid, sc0, se0, cnt,
    snd1, rcv1, snd2, rcv2, snd3, rcv3, snd4, rcv4,
    field, feed,
    a2a_send, a2a_recv, halo_send, halo_recv,
):
    slab = lax.axis_index("slab")
    row = lax.axis_index("row")
    me = slab * 4 + row
    depth = pot.shape[0]
    lines = pot.shape[1]
    cells = volt.shape[1]
    half = depth * lines

    def walk(step):
        d = lax.rem(me + step * WALK, DEVS)
        return d, {"slab": lax.div(d, 4), "row": lax.rem(d, 4)}

    barrier = pltpu.get_barrier_semaphore()

    def greet(step, carry):
        _, where = walk(step)
        pl.semaphore_signal(barrier, inc=1, device_id=where)
        return carry

    edge = (field.shape[0], 1) + field.shape[2:]
    side = (field.shape[0], depth + 2, 8, field.shape[3])

    @pl.when(slab == 0)
    def _():
        field[:, 0:1] = jnp.zeros(edge, F32)

    @pl.when(slab == 31)
    def _():
        field[:, depth + 1:] = jnp.zeros(edge, F32)

    @pl.when(row == 0)
    def _():
        field[:, :, 0:8] = jnp.zeros(side, F32)

    @pl.when(row == 3)
    def _():
        field[:, :, lines + 8:] = jnp.zeros(side, F32)

    lax.fori_loop(1, DEVS, greet, 0)

    field[0, 1:1 + depth, 8:8 + lines] = pot[...]

    owner = tgt[...]
    place = plc[...]
    own = (owner == lax.broadcasted_iota(jnp.int32, (DEVS, cells), 0)).astype(F32)
    ownb = own.astype(BF16)
    earlier = (
        lax.broadcasted_iota(jnp.int32, (cells, cells), 0)
        < lax.broadcasted_iota(jnp.int32, (cells, cells), 1)
    ).astype(F32).astype(BF16)
    before = dot1(ownb, earlier)
    order = jnp.sum(before * own, axis=0, keepdims=True)
    for k in range(CAP):
        ohc[k * DEVS:(k + 1) * DEVS, :] = (own * (order == float(k)).astype(F32)).astype(BF16)
    spot = lax.rem(place, 2) * half + lax.div(place, 2) + 1
    ranks = lax.broadcasted_iota(jnp.int32, (DEVS, cells), 0).astype(F32)
    here = (ranks == order).astype(F32)
    upper = lax.div(spot, 16).astype(F32)
    lower = lax.rem(spot, 16).astype(F32)
    table = 16.0 * dot1(ownb, (here * upper).astype(BF16), BOTH) + dot1(
        ownb, (here * lower).astype(BF16), BOTH
    )
    snd1[pl.ds(CAP, DEVS, stride=SLOT), :] = table

    for k in range(8):
        unit = (
            lax.broadcasted_iota(jnp.int32, (64, 512), 0) + 64 * k
            == lax.broadcasted_iota(jnp.int32, (64, 512), 1)
        ).astype(F32)
        for earlier_block in range(k):
            above = amat[64 * earlier_block:64 * (earlier_block + 1), :]
            unit = unit + jnp.where(
                par[0:1, k - 1:k] == earlier_block, coupling * above, jnp.zeros_like(above)
            )
        amat[64 * k:64 * (k + 1), :] = lax.dot_general(
            inv[k], unit, ROWS, precision=lax.Precision.HIGHEST, preferred_element_type=F32
        )
    weighted = trans[...] * cond[...]
    back = dot3(weighted, amat[...])
    back2 = dot3(back, amat[...])
    cmat = dot3(back - weighted, trans[...], BOTH)
    emat = dot3(back2, trans[...], BOTH)
    coef[0:128, :] = cmat
    coef[128:256, :] = emat

    def to_slots(hot, parts, snd):
        for group in range(CAP // 4):
            got = dot1(hot[group * 512:(group + 1) * 512, :], parts[...])
            got = got[:, 0:128] + got[:, 128:256]
            for k in range(4):
                snd[pl.ds(group * 4 + k, DEVS, stride=SLOT), :] = got[k * 128:(k + 1) * 128]

    def fill(weights, snd):
        made = dot3(weights, volt[...])
        high, low = split(jnp.transpose(made))
        pt[:, 0:128] = high
        pt[:, 128:256] = low
        to_slots(ohc, pt, snd)

    def send_part(number, snd, rcv, rows, first, last):
        def send(step, carry):
            d, where = walk(step)
            pltpu.make_async_remote_copy(
                src_ref=snd.at[pl.ds(pl.multiple_of(d * SLOT, SLOT), rows)],
                dst_ref=rcv.at[pl.ds(pl.multiple_of(me * SLOT, SLOT), rows)],
                send_sem=a2a_send.at[number],
                recv_sem=a2a_recv.at[number],
                device_id=where,
            ).start()
            return carry

        lax.fori_loop(max(first * DEVS // 4, 1), last * DEVS // 4, send, 0)
        if last == 4:
            mine = pl.ds(pl.multiple_of(me * SLOT, SLOT), SLOT)
            rcv[mine, :] = snd[mine, :]

    def arrived(number, rcv, rows):
        total = pl.ds(0, (DEVS - 1) * rows)
        pltpu.make_async_copy(rcv.at[total], rcv.at[total], a2a_recv.at[number]).wait()

    def departed(number, snd, rows):
        total = pl.ds(0, (DEVS - 1) * rows)
        pltpu.make_async_copy(snd.at[total], snd.at[total], a2a_send.at[number]).wait()

    def halo(number, act):
        ref = field.at[number]
        for at, (dz, dy) in enumerate(DIRS):
            inner_z = pl.ds(1, depth)
            inner_y = pl.ds(8, lines)
            if dz:
                src = ref.at[pl.ds(1 if dz < 0 else depth, 1), inner_y]
                dst = ref.at[pl.ds(depth + 1 if dz < 0 else 0, 1), inner_y]
            else:
                src = ref.at[inner_z, pl.ds(8 if dy < 0 else lines, 8)]
                dst = ref.at[inner_z, pl.ds(lines + 8 if dy < 0 else 0, 8)]
            copy = pltpu.make_async_remote_copy(
                src_ref=src,
                dst_ref=dst,
                send_sem=halo_send.at[number * 4 + at],
                recv_sem=halo_recv.at[number * 4 + at],
                device_id={"slab": slab + dz, "row": row + dy},
            )
            to = (slab + dz >= 0) & (slab + dz <= 31) & (row + dy >= 0) & (row + dy <= 3)
            came = (slab - dz >= 0) & (slab - dz <= 31) & (row - dy >= 0) & (row - dy <= 3)
            if act == "start":
                pl.when(to)(copy.start)
            elif act == "recv":
                pl.when(came)(copy.wait_recv)
            else:
                pl.when(to)(copy.wait_send)

    fill(back, snd1)

    pl.semaphore_wait(barrier, DEVS - 1)
    halo(0, "start")
    send_part(0, snd1, rcv1, CAP + 1, 0, 4)
    fill(back2, snd2)
    send_part(1, snd2, rcv2, CAP, 0, 3)

    grid[0:half, :] = pot[:, :, 0:128].reshape(half, 128)
    grid[half:, :] = pot[:, :, 128:256].reshape(half, 128)
    for q in range(4):
        rows_of = pl.ds(q * 512, 512)
        part = grid[rows_of, :]
        sc0[rows_of, :] = dot3(part, coef[0:128, :], BOTH)
        se0[rows_of, :] = dot3(part, coef[128:256, :], BOTH)
    first = dot3(amat[...], trans[...], BOTH)
    second = dot3(amat[...], first)
    ymat[...] = dot3(amat[...], volt[...])
    ymat[...] = dot3(amat[...], ymat[...])

    def rows_in(rcv):
        for k in range(CAP):
            high, low = split(rcv[pl.ds(k, DEVS, stride=SLOT), :])
            zmat[k * DEVS:(k + 1) * DEVS, 0:128] = high
            zmat[k * DEVS:(k + 1) * DEVS, 128:256] = low

    def place_rows(number, q, value):
        z = (q % 2) * 4
        x = (q // 2) * 128
        feed[number, z:z + 4, :, x:x + 128] = value.reshape(4, lines, 128)

    arrived(0, rcv1, CAP + 1)
    asked = rcv1[pl.ds(CAP, DEVS, stride=SLOT), :] - 1.0
    asked_t = jnp.transpose(asked)
    rows_in(rcv1)
    ones = jnp.ones((128, 128), BF16)
    for q in range(4):
        rows_of = pl.ds(q * 512, 512)
        spots = (lax.broadcasted_iota(jnp.int32, (512, 128), 0) + q * 512).astype(F32)
        many = jnp.zeros((512, 128), F32)
        for k in range(CAP):
            hit = (asked_t[k:k + 1, :] == spots).astype(F32)
            many = many + hit
            ohp[rows_of, k * 128:(k + 1) * 128] = hit.astype(BF16)
        count = dot1(many.astype(BF16), ones)
        cnt[rows_of, :] = count
        got = dot1(ohp[rows_of, :], zmat[...])
        place_rows(0, q, got[:, 0:128] + got[:, 128:256] + count * sc0[rows_of, :])
    def table_of_asked():
        for q in range(4):
            spots = (lax.broadcasted_iota(jnp.int32, (128, 512), 1) + q * 512).astype(F32)
            for k in range(CAP):
                hit = (asked[:, k:k + 1] == spots).astype(F32)
                oht[k * 128:(k + 1) * 128, q * 512:(q + 1) * 512] = hit.astype(BF16)

    def gather(snd):
        high, low = split(grid[...])
        gmat[:, 0:128] = high
        gmat[:, 128:256] = low
        to_slots(oht, gmat, snd)

    lane = lax.broadcasted_iota(jnp.int32, (8, 128), 1)
    line = lax.broadcasted_iota(jnp.int32, (8, 128), 0)
    zero = jnp.zeros((8, 128), F32)
    tiles = lines // 8

    def sweep(number):
        src = field.at[number]
        last = number + 1 == 2 * SWEEPS

        def tile(at_z, t, h):
            return src[at_z, 8 * t + 8:8 * t + 16, 128 * h:128 * h + 128]

        def strip(z, which):
            for t in which:
                left, right = tile(z, t, 0), tile(z, t, 1)
                before_x = (jnp.where(lane == 127, zero, left), jnp.where(lane == 127, left, right))
                after_x = (jnp.where(lane == 0, right, left), jnp.where(lane == 0, zero, right))
                for h, mid in enumerate((left, right)):
                    x = slice(128 * h, 128 * h + 128)
                    total = tile(z - 1, t, h) + tile(z + 1, t, h)
                    total = total + feed[number // SWEEPS, z - 1, 8 * t:8 * t + 8, x]
                    total = total + (
                        pltpu.roll(jnp.where(line == 7, tile(z, t - 1, h), mid), 1, 0)
                        + pltpu.roll(jnp.where(line == 0, tile(z, t + 1, h), mid), 7, 0)
                    )
                    total = total + (
                        pltpu.roll(before_x[h], 1, 1) + pltpu.roll(after_x[h], 127, 1)
                    )
                    if last:
                        pot_out[z - 1, 8 * t:8 * t + 8, x] = total * scale
                    else:
                        field[number + 1, z, 8 * t + 8:8 * t + 16, x] = total * scale

        def over(first, count, step, which):
            def body(i, carry):
                strip(first + i * step, which)
                return carry

            lax.fori_loop(0, count, body, 0)

        halo(number, "recv")
        if last:
            over(1, depth, 1, range(tiles))
        else:
            over(1, 2, depth - 1, range(tiles))
            over(2, depth - 2, 1, (0, tiles - 1))
            halo(number + 1, "start")
            over(2, depth - 2, 1, range(1, tiles - 1))

    def bring(number, rcv):
        arrived(number, rcv, CAP)
        for k in range(CAP):
            high, low = split(jnp.transpose(rcv[pl.ds(k, DEVS, stride=SLOT), :]))
            lt[0:128, k * 128:(k + 1) * 128] = high
            lt[128:256, k * 128:(k + 1) * 128] = low
        got = dot1(lt[...], ohc[...])
        return got[0:128, :] + got[128:256, :]

    sweep(0)
    send_part(1, snd2, rcv2, CAP, 3, 4)
    table_of_asked()
    gather(snd3)
    sweep(1)
    send_part(2, snd3, rcv3, CAP, 0, 1)
    sweep(2)
    send_part(2, snd3, rcv3, CAP, 1, 2)
    sweep(3)
    send_part(2, snd3, rcv3, CAP, 2, 4)
    for z in range(depth):
        now = field[SWEEPS, 1 + z, 8:8 + lines, :]
        grid[z * lines:(z + 1) * lines, :] = now[:, 0:128]
        grid[half + z * lines:half + (z + 1) * lines, :] = now[:, 128:256]
    for q in range(4):
        rows_of = pl.ds(q * 512, 512)
        se0[rows_of, :] = cnt[rows_of, :] * (
            se0[rows_of, :] + dot3(grid[rows_of, :], coef[0:128, :], BOTH)
        )
    arrived(1, rcv2, CAP)
    rows_in(rcv2)
    for q in range(4):
        rows_of = pl.ds(q * 512, 512)
        got = dot1(ohp[rows_of, :], zmat[...])
        place_rows(1, q, got[:, 0:128] + got[:, 128:256] + se0[rows_of, :])
    sweep(4)
    gather(snd4)
    send_part(3, snd4, rcv4, CAP, 0, 2)
    sweep(5)
    send_part(3, snd4, rcv4, CAP, 2, 3)
    volt_out[...] = ymat[...] + dot3(second, bring(2, rcv3))
    first_out[...] = first
    sweep(6)
    send_part(3, snd4, rcv4, CAP, 3, 4)
    sweep(7)
    seen_out[...] = bring(3, rcv4)
    departed(0, snd1, CAP + 1)
    departed(1, snd2, CAP)
    departed(2, snd3, CAP)
    departed(3, snd4, CAP)
    for number in range(2 * SWEEPS):
        halo(number, "sent")


def finish(held, first, seen, out):
    out[...] = held[...] + dot3(first[...], seen[...])


def shards(voltage, potential, transfer, conductance, inverses, parents, target, place):
    cells = voltage.shape[1]
    depth, lines, wide = potential.shape
    tall = (2 * SWEEPS, depth + 2, lines + 16, wide)
    vmem = pl.BlockSpec(memory_space=pltpu.VMEM)
    block = pltpu.VMEM((DEVS * SLOT, 128), F32)
    held, potential, first, seen = pl.pallas_call(
        kernel,
        out_shape=(
            jax.ShapeDtypeStruct(voltage.shape, F32),
            jax.ShapeDtypeStruct(potential.shape, F32),
            jax.ShapeDtypeStruct((512, 128), F32),
            jax.ShapeDtypeStruct((128, cells), F32),
        ),
        in_specs=[vmem] * 8,
        out_specs=(vmem,) * 4,
        scratch_shapes=[
            pltpu.VMEM((CAP * DEVS, cells), BF16),
            pltpu.VMEM((depth * lines * 2, CAP * DEVS), BF16),
            pltpu.VMEM((CAP * DEVS, depth * lines * 2), BF16),
            pltpu.VMEM((depth * lines * 2, 256), BF16),
            pltpu.VMEM((512, 512), F32),
            pltpu.VMEM((512, cells), F32),
            pltpu.VMEM((256, 128), F32),
            pltpu.VMEM((cells, 256), BF16),
            pltpu.VMEM((CAP * DEVS, 256), BF16),
            pltpu.VMEM((256, CAP * DEVS), BF16),
            pltpu.VMEM((depth * lines * 2, 128), F32),
            pltpu.VMEM((depth * lines * 2, 128), F32),
            pltpu.VMEM((depth * lines * 2, 128), F32),
            pltpu.VMEM((depth * lines * 2, 128), F32),
        ]
        + [block] * 8
        + [pltpu.VMEM(tall, F32), pltpu.VMEM((2, depth, lines, wide), F32)]
        + [
            pltpu.SemaphoreType.DMA((4,)),
            pltpu.SemaphoreType.DMA((4,)),
            pltpu.SemaphoreType.DMA((32,)),
            pltpu.SemaphoreType.DMA((32,)),
        ],
        compiler_params=pltpu.CompilerParams(
            collective_id=0, has_side_effects=True, vmem_limit_bytes=60 * 1024 * 1024
        ),
    )(
        voltage, potential, transfer, conductance.reshape(1, -1), inverses, parents.reshape(1, -1),
        target.reshape(1, -1), place.reshape(1, -1),
    )
    width = 256
    voltage = pl.pallas_call(
        finish,
        grid=(cells // width,),
        out_shape=jax.ShapeDtypeStruct(held.shape, F32),
        in_specs=[
            pl.BlockSpec((512, width), lambda i: (0, i)),
            pl.BlockSpec((512, 128), lambda i: (0, 0)),
            pl.BlockSpec((128, width), lambda i: (0, i)),
        ],
        out_specs=pl.BlockSpec((512, width), lambda i: (0, i)),
    )(held, first, seen)
    return voltage, potential


def solution(mesh):
    return jax.shard_map(
        shards,
        mesh=mesh,
        in_specs=(
            P(None, ("slab", "row")),
            P("slab", "row", None),
            P(),
            P(),
            P(),
            P(),
            P(("slab", "row"), None),
            P(("slab", "row")),
        ),
        out_specs=(P(None, ("slab", "row")), P("slab", "row", None)),
        check_vma=False,
    )
```

```python
import jax
import jax.numpy as jnp
from jax import lax
from jax.experimental import pallas as pl
from jax.experimental.pallas import tpu as pltpu
from jax.sharding import PartitionSpec as P

SWEEPS = 4
CAP = 12
SLOT = 16
DEVS = 128
WALK = 37
scale = 1.0 / 6.25
coupling = 0.5
F32 = jnp.float32
BF16 = jnp.bfloat16
ROWS = (((1,), (0,)), ((), ()))
BOTH = (((1,), (1,)), ((), ()))
DIRS = ((-1, 0), (1, 0), (0, -1), (0, 1))


def split(value):
    high = value.astype(BF16)
    return high, (value - high.astype(F32)).astype(BF16)


def dot1(a, b, dims=ROWS):
    return lax.dot_general(a, b, dims, preferred_element_type=F32)


def dot3(a, b, dims=ROWS):
    ah, al = split(a)
    bh, bl = split(b)
    return dot1(ah, bh, dims) + (dot1(ah, bl, dims) + dot1(al, bh, dims))


def kernel(
    volt, pot, trans, cond, inv, par, tgt, plc, volt_out, pot_out, first_out, seen_out,
    ohc, ohp, oht, gmat, amat, ymat, coef, pt, zmat, lt, grid, sc0, se0, cnt,
    sndi, rcvi, snd1, rcv1, snd2, rcv2, snd3, rcv3, snd4, rcv4,
    field, feed,
    a2a_send, a2a_recv, halo_send, halo_recv,
):
    slab = lax.axis_index("slab")
    row = lax.axis_index("row")
    me = slab * 4 + row
    depth = pot.shape[0]
    lines = pot.shape[1]
    cells = volt.shape[1]
    half = depth * lines

    def walk(step):
        d = lax.rem(me + step * WALK, DEVS)
        return d, {"slab": lax.div(d, 4), "row": lax.rem(d, 4)}

    barrier = pltpu.get_barrier_semaphore()

    def greet(step, carry):
        _, where = walk(step)
        pl.semaphore_signal(barrier, inc=1, device_id=where)
        return carry

    edge = (field.shape[0], 1) + field.shape[2:]
    side = (field.shape[0], depth + 2, 8, field.shape[3])

    @pl.when(slab == 0)
    def _():
        field[:, 0:1] = jnp.zeros(edge, F32)

    @pl.when(slab == 31)
    def _():
        field[:, depth + 1:] = jnp.zeros(edge, F32)

    @pl.when(row == 0)
    def _():
        field[:, :, 0:8] = jnp.zeros(side, F32)

    @pl.when(row == 3)
    def _():
        field[:, :, lines + 8:] = jnp.zeros(side, F32)

    lax.fori_loop(1, DEVS, greet, 0)

    field[0, 1:1 + depth, 8:8 + lines] = pot[...]

    owner = tgt[...]
    place = plc[...].reshape(1, cells)
    own = (owner == lax.broadcasted_iota(jnp.int32, (DEVS, cells), 0)).astype(F32)
    ownb = own.astype(BF16)
    earlier = (
        lax.broadcasted_iota(jnp.int32, (cells, cells), 0)
        < lax.broadcasted_iota(jnp.int32, (cells, cells), 1)
    ).astype(F32).astype(BF16)
    before = dot1(ownb, earlier)
    order = jnp.sum(before * own, axis=0, keepdims=True)
    for k in range(CAP):
        ohc[k * DEVS:(k + 1) * DEVS, :] = (own * (order == float(k)).astype(F32)).astype(BF16)
    spot = lax.rem(place, 2) * half + lax.div(place, 2) + 1
    ranks = lax.broadcasted_iota(jnp.int32, (DEVS, cells), 0).astype(F32)
    here = (ranks == order).astype(F32)
    upper = lax.div(spot, 16).astype(F32)
    lower = lax.rem(spot, 16).astype(F32)
    table = 16.0 * dot1(ownb, (here * upper).astype(BF16), BOTH) + dot1(
        ownb, (here * lower).astype(BF16), BOTH
    )
    sndi[pl.ds(0, DEVS, stride=8), :] = table

    for k in range(8):
        unit = (
            lax.broadcasted_iota(jnp.int32, (64, 512), 0) + 64 * k
            == lax.broadcasted_iota(jnp.int32, (64, 512), 1)
        ).astype(F32)
        for earlier_block in range(k):
            above = amat[64 * earlier_block:64 * (earlier_block + 1), :]
            unit = unit + jnp.where(
                par[0:1, k - 1:k] == earlier_block, coupling * above, jnp.zeros_like(above)
            )
        amat[64 * k:64 * (k + 1), :] = lax.dot_general(
            inv[k], unit, ROWS, precision=lax.Precision.HIGHEST, preferred_element_type=F32
        )
    weighted = trans[...] * cond[...]
    back = dot3(weighted, amat[...])
    back2 = dot3(back, amat[...])
    cmat = dot3(back - weighted, trans[...], BOTH)
    emat = dot3(back2, trans[...], BOTH)
    coef[0:128, :] = cmat
    coef[128:256, :] = emat

    def to_slots(hot, parts, snd):
        for group in range(CAP // 4):
            got = dot1(hot[group * 512:(group + 1) * 512, :], parts[...])
            got = got[:, 0:128] + got[:, 128:256]
            for k in range(4):
                snd[pl.ds(group * 4 + k, DEVS, stride=SLOT), :] = got[k * 128:(k + 1) * 128]

    def fill(weights, snd):
        made = dot3(weights, volt[...])
        high, low = split(jnp.transpose(made))
        pt[:, 0:128] = high
        pt[:, 128:256] = low
        to_slots(ohc, pt, snd)

    def send_part(number, snd, rcv, rows, first, last, slot=SLOT):
        def send(step, carry):
            d, where = walk(step)
            pltpu.make_async_remote_copy(
                src_ref=snd.at[pl.ds(pl.multiple_of(d * slot, slot), rows)],
                dst_ref=rcv.at[pl.ds(pl.multiple_of(me * slot, slot), rows)],
                send_sem=a2a_send.at[number],
                recv_sem=a2a_recv.at[number],
                device_id=where,
            ).start()
            return carry

        lax.fori_loop(max(first * DEVS // 4, 1), last * DEVS // 4, send, 0)
        if last == 4:
            mine = pl.ds(pl.multiple_of(me * slot, slot), slot)
            rcv[mine, :] = snd[mine, :]

    def arrived(number, rcv, rows):
        total = pl.ds(0, (DEVS - 1) * rows)
        pltpu.make_async_copy(rcv.at[total], rcv.at[total], a2a_recv.at[number]).wait()

    def departed(number, snd, rows):
        total = pl.ds(0, (DEVS - 1) * rows)
        pltpu.make_async_copy(snd.at[total], snd.at[total], a2a_send.at[number]).wait()

    def halo(number, act):
        ref = field.at[number]
        for at, (dz, dy) in enumerate(DIRS):
            inner_z = pl.ds(1, depth)
            inner_y = pl.ds(8, lines)
            if dz:
                src = ref.at[pl.ds(1 if dz < 0 else depth, 1), inner_y]
                dst = ref.at[pl.ds(depth + 1 if dz < 0 else 0, 1), inner_y]
            else:
                src = ref.at[inner_z, pl.ds(8 if dy < 0 else lines, 8)]
                dst = ref.at[inner_z, pl.ds(lines + 8 if dy < 0 else 0, 8)]
            copy = pltpu.make_async_remote_copy(
                src_ref=src,
                dst_ref=dst,
                send_sem=halo_send.at[number * 4 + at],
                recv_sem=halo_recv.at[number * 4 + at],
                device_id={"slab": slab + dz, "row": row + dy},
            )
            to = (slab + dz >= 0) & (slab + dz <= 31) & (row + dy >= 0) & (row + dy <= 3)
            came = (slab - dz >= 0) & (slab - dz <= 31) & (row - dy >= 0) & (row - dy <= 3)
            if act == "start":
                pl.when(to)(copy.start)
            elif act == "recv":
                pl.when(came)(copy.wait_recv)
            else:
                pl.when(to)(copy.wait_send)

    fill(back, snd1)

    pl.semaphore_wait(barrier, DEVS - 1)
    halo(0, "start")
    send_part(4, sndi, rcvi, 1, 0, 4, 8)
    send_part(0, snd1, rcv1, CAP, 0, 4)
    fill(back2, snd2)
    send_part(1, snd2, rcv2, CAP, 0, 3)

    grid[0:half, :] = pot[:, :, 0:128].reshape(half, 128)
    grid[half:, :] = pot[:, :, 128:256].reshape(half, 128)
    for q in range(4):
        rows_of = pl.ds(q * 512, 512)
        part = grid[rows_of, :]
        sc0[rows_of, :] = dot3(part, coef[0:128, :], BOTH)
        se0[rows_of, :] = dot3(part, coef[128:256, :], BOTH)
    def rows_in(rcv):
        for k in range(CAP):
            high, low = split(rcv[pl.ds(k, DEVS, stride=SLOT), :])
            zmat[k * DEVS:(k + 1) * DEVS, 0:128] = high
            zmat[k * DEVS:(k + 1) * DEVS, 128:256] = low

    def place_rows(number, q, value):
        z = (q % 2) * 4
        x = (q // 2) * 128
        feed[number, z:z + 4, :, x:x + 128] = value.reshape(4, lines, 128)

    arrived(4, rcvi, 1)
    asked = rcvi[pl.ds(0, DEVS, stride=8), :] - 1.0
    asked_t = jnp.transpose(asked)
    ones = jnp.ones((128, 128), BF16)
    for q in range(4):
        rows_of = pl.ds(q * 512, 512)
        spots = (lax.broadcasted_iota(jnp.int32, (512, 128), 0) + q * 512).astype(F32)
        many = jnp.zeros((512, 128), F32)
        for k in range(CAP):
            hit = (asked_t[k:k + 1, :] == spots).astype(F32)
            many = many + hit
            ohp[rows_of, k * 128:(k + 1) * 128] = hit.astype(BF16)
        count = dot1(many.astype(BF16), ones)
        cnt[rows_of, :] = count
        sc0[rows_of, :] = count * sc0[rows_of, :]

    def table_of_asked():
        for q in range(4):
            spots = (lax.broadcasted_iota(jnp.int32, (128, 512), 1) + q * 512).astype(F32)
            for k in range(CAP):
                hit = (asked[:, k:k + 1] == spots).astype(F32)
                oht[k * 128:(k + 1) * 128, q * 512:(q + 1) * 512] = hit.astype(BF16)

    def gather(snd):
        high, low = split(grid[...])
        gmat[:, 0:128] = high
        gmat[:, 128:256] = low
        to_slots(oht, gmat, snd)

    table_of_asked()
    gather(snd3)
    first = dot3(amat[...], trans[...], BOTH)
    second = dot3(amat[...], first)
    arrived(0, rcv1, CAP)
    rows_in(rcv1)
    for q in range(4):
        rows_of = pl.ds(q * 512, 512)
        got = dot1(ohp[rows_of, :], zmat[...])
        place_rows(0, q, got[:, 0:128] + got[:, 128:256] + sc0[rows_of, :])

    lane = lax.broadcasted_iota(jnp.int32, (8, 128), 1)
    line = lax.broadcasted_iota(jnp.int32, (8, 128), 0)
    zero = jnp.zeros((8, 128), F32)
    tiles = lines // 8

    def sweep(number):
        src = field.at[number]
        last = number + 1 == 2 * SWEEPS

        def tile(at_z, t, h):
            return src[at_z, 8 * t + 8:8 * t + 16, 128 * h:128 * h + 128]

        def strip(z, which):
            for t in which:
                left, right = tile(z, t, 0), tile(z, t, 1)
                before_x = (jnp.where(lane == 127, zero, left), jnp.where(lane == 127, left, right))
                after_x = (jnp.where(lane == 0, right, left), jnp.where(lane == 0, zero, right))
                for h, mid in enumerate((left, right)):
                    x = slice(128 * h, 128 * h + 128)
                    total = tile(z - 1, t, h) + tile(z + 1, t, h)
                    total = total + feed[number // SWEEPS, z - 1, 8 * t:8 * t + 8, x]
                    total = total + (
                        pltpu.roll(jnp.where(line == 7, tile(z, t - 1, h), mid), 1, 0)
                        + pltpu.roll(jnp.where(line == 0, tile(z, t + 1, h), mid), 7, 0)
                    )
                    total = total + (
                        pltpu.roll(before_x[h], 1, 1) + pltpu.roll(after_x[h], 127, 1)
                    )
                    if last:
                        pot_out[z - 1, 8 * t:8 * t + 8, x] = total * scale
                    else:
                        field[number + 1, z, 8 * t + 8:8 * t + 16, x] = total * scale

        def over(first, count, step, which):
            def body(i, carry):
                strip(first + i * step, which)
                return carry

            lax.fori_loop(0, count, body, 0)

        halo(number, "recv")
        if last:
            over(1, depth, 1, range(tiles))
        else:
            over(1, 2, depth - 1, range(tiles))
            over(2, depth - 2, 1, (0, tiles - 1))
            halo(number + 1, "start")
            over(2, depth - 2, 1, range(1, tiles - 1))

    def bring(number, rcv):
        arrived(number, rcv, CAP)
        for k in range(CAP):
            high, low = split(jnp.transpose(rcv[pl.ds(k, DEVS, stride=SLOT), :]))
            lt[0:128, k * 128:(k + 1) * 128] = high
            lt[128:256, k * 128:(k + 1) * 128] = low
        got = dot1(lt[...], ohc[...])
        return got[0:128, :] + got[128:256, :]

    sweep(0)
    send_part(1, snd2, rcv2, CAP, 3, 4)
    ymat[...] = dot3(amat[...], volt[...])
    sweep(1)
    send_part(2, snd3, rcv3, CAP, 0, 1)
    ymat[...] = dot3(amat[...], ymat[...])
    sweep(2)
    send_part(2, snd3, rcv3, CAP, 1, 2)
    sweep(3)
    send_part(2, snd3, rcv3, CAP, 2, 4)
    for z in range(depth):
        now = field[SWEEPS, 1 + z, 8:8 + lines, :]
        grid[z * lines:(z + 1) * lines, :] = now[:, 0:128]
        grid[half + z * lines:half + (z + 1) * lines, :] = now[:, 128:256]
    for q in range(4):
        rows_of = pl.ds(q * 512, 512)
        se0[rows_of, :] = cnt[rows_of, :] * (
            se0[rows_of, :] + dot3(grid[rows_of, :], coef[0:128, :], BOTH)
        )
    arrived(1, rcv2, CAP)
    rows_in(rcv2)
    for q in range(4):
        rows_of = pl.ds(q * 512, 512)
        got = dot1(ohp[rows_of, :], zmat[...])
        place_rows(1, q, got[:, 0:128] + got[:, 128:256] + se0[rows_of, :])
    sweep(4)
    gather(snd4)
    send_part(3, snd4, rcv4, CAP, 0, 2)
    sweep(5)
    send_part(3, snd4, rcv4, CAP, 2, 3)
    volt_out[...] = ymat[...] + dot3(second, bring(2, rcv3))
    high, low = split(first)
    first_out[:, 0:128] = high
    first_out[:, 128:256] = high
    first_out[:, 256:384] = low
    sweep(6)
    send_part(3, snd4, rcv4, CAP, 3, 4)
    sweep(7)
    high, low = split(bring(3, rcv4))
    seen_out[0:128, :] = high
    seen_out[128:256, :] = low
    seen_out[256:384, :] = high
    departed(0, snd1, CAP)
    departed(4, sndi, 1)
    departed(1, snd2, CAP)
    departed(2, snd3, CAP)
    departed(3, snd4, CAP)
    for number in range(2 * SWEEPS):
        halo(number, "sent")


def finish(held, first, seen, out):
    out[...] = held[...] + dot1(first[...], seen[...])


def shards(voltage, potential, transfer, conductance, inverses, parents, target, place):
    cells = voltage.shape[1]
    depth, lines, wide = potential.shape
    tall = (2 * SWEEPS, depth + 2, lines + 16, wide)
    vmem = pl.BlockSpec(memory_space=pltpu.VMEM)
    block = pltpu.VMEM((DEVS * SLOT, 128), F32)
    held, potential, first, seen = pl.pallas_call(
        kernel,
        out_shape=(
            jax.ShapeDtypeStruct(voltage.shape, F32),
            jax.ShapeDtypeStruct(potential.shape, F32),
            jax.ShapeDtypeStruct((512, 384), BF16),
            jax.ShapeDtypeStruct((384, cells), BF16),
        ),
        in_specs=[vmem] * 8,
        out_specs=(vmem,) * 4,
        scratch_shapes=[
            pltpu.VMEM((CAP * DEVS, cells), BF16),
            pltpu.VMEM((depth * lines * 2, CAP * DEVS), BF16),
            pltpu.VMEM((CAP * DEVS, depth * lines * 2), BF16),
            pltpu.VMEM((depth * lines * 2, 256), BF16),
            pltpu.VMEM((512, 512), F32),
            pltpu.VMEM((512, cells), F32),
            pltpu.VMEM((256, 128), F32),
            pltpu.VMEM((cells, 256), BF16),
            pltpu.VMEM((CAP * DEVS, 256), BF16),
            pltpu.VMEM((256, CAP * DEVS), BF16),
            pltpu.VMEM((depth * lines * 2, 128), F32),
            pltpu.VMEM((depth * lines * 2, 128), F32),
            pltpu.VMEM((depth * lines * 2, 128), F32),
            pltpu.VMEM((depth * lines * 2, 128), F32),
        ]
        + [pltpu.VMEM((DEVS * 8, 128), F32)] * 2
        + [block] * 8
        + [pltpu.VMEM(tall, F32), pltpu.VMEM((2, depth, lines, wide), F32)]
        + [
            pltpu.SemaphoreType.DMA((5,)),
            pltpu.SemaphoreType.DMA((5,)),
            pltpu.SemaphoreType.DMA((32,)),
            pltpu.SemaphoreType.DMA((32,)),
        ],
        compiler_params=pltpu.CompilerParams(
            collective_id=0, has_side_effects=True, vmem_limit_bytes=60 * 1024 * 1024
        ),
    )(
        voltage, potential, transfer, conductance.reshape(1, -1), inverses, parents.reshape(1, -1),
        target.reshape(1, -1), place,
    )
    width = 256
    voltage = pl.pallas_call(
        finish,
        grid=(cells // width,),
        out_shape=jax.ShapeDtypeStruct(held.shape, F32),
        in_specs=[
            pl.BlockSpec((512, width), lambda i: (0, i)),
            pl.BlockSpec((512, 384), lambda i: (0, 0)),
            pl.BlockSpec((384, width), lambda i: (0, i)),
        ],
        out_specs=pl.BlockSpec((512, width), lambda i: (0, i)),
    )(held, first, seen)
    return voltage, potential


def solution(mesh):
    return jax.shard_map(
        shards,
        mesh=mesh,
        in_specs=(
            P(None, ("slab", "row")),
            P("slab", "row", None),
            P(),
            P(),
            P(),
            P(),
            P(("slab", "row"), None),
            P(("slab", "row")),
        ),
        out_specs=(P(None, ("slab", "row")), P("slab", "row", None)),
        check_vma=False,
    )
```

```python
import jax
import jax.numpy as jnp
from jax import lax
from jax.experimental import pallas as pl
from jax.experimental.pallas import tpu as pltpu
from jax.sharding import PartitionSpec as P

SWEEPS = 4
CAP = 12
SLOT = 16
DEVS = 128
WALK = 37
scale = 1.0 / 6.25
coupling = 0.5
F32 = jnp.float32
BF16 = jnp.bfloat16
ROWS = (((1,), (0,)), ((), ()))
BOTH = (((1,), (1,)), ((), ()))
DIRS = ((-1, 0), (1, 0), (0, -1), (0, 1))


def split(value):
    high = value.astype(BF16)
    return high, (value - high.astype(F32)).astype(BF16)


def dot1(a, b, dims=ROWS):
    return lax.dot_general(a, b, dims, preferred_element_type=F32)


def dot3(a, b, dims=ROWS):
    ah, al = split(a)
    bh, bl = split(b)
    return dot1(ah, bh, dims) + (dot1(ah, bl, dims) + dot1(al, bh, dims))


def kernel(
    volt, pot, trans, cond, inv, par, tgt, plc, volt_out, pot_out, first_out, seen_out,
    ohc, ohp, oht, gmat, amat, ymat, coef, pt, zmat, lt, grid, sc0, se0, cnt,
    sndi, rcvi, snd1, rcv1, snd2, rcv2, snd3, rcv3, snd4, rcv4,
    field, feed,
    a2a_send, a2a_recv, halo_send, halo_recv,
):
    slab = lax.axis_index("slab")
    row = lax.axis_index("row")
    me = slab * 4 + row
    depth = pot.shape[0]
    lines = pot.shape[1]
    cells = volt.shape[1]
    half = depth * lines

    def walk(step):
        d = lax.rem(me + step * WALK, DEVS)
        return d, {"slab": lax.div(d, 4), "row": lax.rem(d, 4)}

    barrier = pltpu.get_barrier_semaphore()

    def greet(step, carry):
        _, where = walk(step)
        pl.semaphore_signal(barrier, inc=1, device_id=where)
        return carry

    edge = (field.shape[0], 1) + field.shape[2:]
    side = (field.shape[0], depth + 2, 8, field.shape[3])

    @pl.when(slab == 0)
    def _():
        field[:, 0:1] = jnp.zeros(edge, F32)

    @pl.when(slab == 31)
    def _():
        field[:, depth + 1:] = jnp.zeros(edge, F32)

    @pl.when(row == 0)
    def _():
        field[:, :, 0:8] = jnp.zeros(side, F32)

    @pl.when(row == 3)
    def _():
        field[:, :, lines + 8:] = jnp.zeros(side, F32)

    lax.fori_loop(1, DEVS, greet, 0)

    field[0, 1:1 + depth, 8:8 + lines] = pot[...]

    owner = tgt[...]
    place = plc[...].reshape(1, cells)
    own = (owner == lax.broadcasted_iota(jnp.int32, (DEVS, cells), 0)).astype(F32)
    ownb = own.astype(BF16)
    earlier = (
        lax.broadcasted_iota(jnp.int32, (cells, cells), 0)
        < lax.broadcasted_iota(jnp.int32, (cells, cells), 1)
    ).astype(F32).astype(BF16)
    before = dot1(ownb, earlier)
    order = jnp.sum(before * own, axis=0, keepdims=True)
    for k in range(CAP):
        ohc[k * DEVS:(k + 1) * DEVS, :] = (own * (order == float(k)).astype(F32)).astype(BF16)
    spot = lax.rem(place, 2) * half + lax.div(place, 2) + 1
    ranks = lax.broadcasted_iota(jnp.int32, (DEVS, cells), 0).astype(F32)
    here = (ranks == order).astype(F32)
    upper = lax.div(spot, 16).astype(F32)
    lower = lax.rem(spot, 16).astype(F32)
    table = 16.0 * dot1(ownb, (here * upper).astype(BF16), BOTH) + dot1(
        ownb, (here * lower).astype(BF16), BOTH
    )
    sndi[pl.ds(0, DEVS, stride=8), :] = table

    for k in range(8):
        unit = (
            lax.broadcasted_iota(jnp.int32, (64, 512), 0) + 64 * k
            == lax.broadcasted_iota(jnp.int32, (64, 512), 1)
        ).astype(F32)
        for earlier_block in range(k):
            above = amat[64 * earlier_block:64 * (earlier_block + 1), :]
            unit = unit + jnp.where(
                par[0:1, k - 1:k] == earlier_block, coupling * above, jnp.zeros_like(above)
            )
        amat[64 * k:64 * (k + 1), :] = lax.dot_general(
            inv[k], unit, ROWS, precision=lax.Precision.HIGHEST, preferred_element_type=F32
        )
    weighted = trans[...] * cond[...]
    back = dot3(weighted, amat[...])
    back2 = dot3(back, amat[...])
    cmat = dot3(back - weighted, trans[...], BOTH)
    emat = dot3(back2, trans[...], BOTH)
    coef[0:128, :] = cmat
    coef[128:256, :] = emat

    def to_slots(hot, parts, snd):
        for group in range(CAP // 4):
            got = dot1(hot[group * 512:(group + 1) * 512, :], parts[...])
            got = got[:, 0:128] + got[:, 128:256]
            for k in range(4):
                snd[pl.ds(group * 4 + k, DEVS, stride=SLOT), :] = got[k * 128:(k + 1) * 128]

    def fill(weights, snd):
        made = dot3(weights, volt[...])
        high, low = split(jnp.transpose(made))
        pt[:, 0:128] = high
        pt[:, 128:256] = low
        to_slots(ohc, pt, snd)

    def send_part(number, snd, rcv, rows, first, last, slot=SLOT):
        def send(step, carry):
            d, where = walk(step)
            pltpu.make_async_remote_copy(
                src_ref=snd.at[pl.ds(pl.multiple_of(d * slot, slot), rows)],
                dst_ref=rcv.at[pl.ds(pl.multiple_of(me * slot, slot), rows)],
                send_sem=a2a_send.at[number],
                recv_sem=a2a_recv.at[number],
                device_id=where,
            ).start()
            return carry

        lax.fori_loop(max(first * DEVS // 4, 1), last * DEVS // 4, send, 0)
        if last == 4:
            mine = pl.ds(pl.multiple_of(me * slot, slot), slot)
            rcv[mine, :] = snd[mine, :]

    def arrived(number, rcv, rows):
        total = pl.ds(0, (DEVS - 1) * rows)
        pltpu.make_async_copy(rcv.at[total], rcv.at[total], a2a_recv.at[number]).wait()

    def departed(number, snd, rows):
        total = pl.ds(0, (DEVS - 1) * rows)
        pltpu.make_async_copy(snd.at[total], snd.at[total], a2a_send.at[number]).wait()

    def halo(number, act):
        ref = field.at[number]
        for at, (dz, dy) in enumerate(DIRS):
            inner_z = pl.ds(1, depth)
            inner_y = pl.ds(8, lines)
            if dz:
                src = ref.at[pl.ds(1 if dz < 0 else depth, 1), inner_y]
                dst = ref.at[pl.ds(depth + 1 if dz < 0 else 0, 1), inner_y]
            else:
                src = ref.at[inner_z, pl.ds(8 if dy < 0 else lines, 8)]
                dst = ref.at[inner_z, pl.ds(lines + 8 if dy < 0 else 0, 8)]
            copy = pltpu.make_async_remote_copy(
                src_ref=src,
                dst_ref=dst,
                send_sem=halo_send.at[number * 4 + at],
                recv_sem=halo_recv.at[number * 4 + at],
                device_id={"slab": slab + dz, "row": row + dy},
            )
            to = (slab + dz >= 0) & (slab + dz <= 31) & (row + dy >= 0) & (row + dy <= 3)
            came = (slab - dz >= 0) & (slab - dz <= 31) & (row - dy >= 0) & (row - dy <= 3)
            if act == "start":
                pl.when(to)(copy.start)
            elif act == "recv":
                pl.when(came)(copy.wait_recv)
            else:
                pl.when(to)(copy.wait_send)

    fill(back, snd1)

    pl.semaphore_wait(barrier, DEVS - 1)
    halo(0, "start")
    send_part(4, sndi, rcvi, 1, 0, 4, 8)
    send_part(0, snd1, rcv1, CAP, 0, 4)
    fill(back2, snd2)
    send_part(1, snd2, rcv2, CAP, 0, 3)

    grid[0:half, :] = pot[:, :, 0:128].reshape(half, 128)
    grid[half:, :] = pot[:, :, 128:256].reshape(half, 128)
    for q in range(4):
        rows_of = pl.ds(q * 512, 512)
        part = grid[rows_of, :]
        sc0[rows_of, :] = dot3(part, coef[0:128, :], BOTH)
        se0[rows_of, :] = dot3(part, coef[128:256, :], BOTH)
    def rows_in(rcv):
        for k in range(CAP):
            high, low = split(rcv[pl.ds(k, DEVS, stride=SLOT), :])
            zmat[k * DEVS:(k + 1) * DEVS, 0:128] = high
            zmat[k * DEVS:(k + 1) * DEVS, 128:256] = low

    def place_rows(number, q, value):
        z = (q % 2) * 4
        x = (q // 2) * 128
        feed[number, z:z + 4, :, x:x + 128] = value.reshape(4, lines, 128)

    arrived(4, rcvi, 1)
    asked = rcvi[pl.ds(0, DEVS, stride=8), :] - 1.0
    asked_t = jnp.transpose(asked)
    ones = jnp.ones((128, 128), BF16)
    for q in range(4):
        rows_of = pl.ds(q * 512, 512)
        spots = (lax.broadcasted_iota(jnp.int32, (512, 128), 0) + q * 512).astype(F32)
        many = jnp.zeros((512, 128), F32)
        for k in range(CAP):
            hit = (asked_t[k:k + 1, :] == spots).astype(F32)
            many = many + hit
            ohp[rows_of, k * 128:(k + 1) * 128] = hit.astype(BF16)
        count = dot1(many.astype(BF16), ones)
        cnt[rows_of, :] = count
        sc0[rows_of, :] = count * sc0[rows_of, :]

    def table_of_asked():
        for q in range(4):
            spots = (lax.broadcasted_iota(jnp.int32, (128, 512), 1) + q * 512).astype(F32)
            for k in range(CAP):
                hit = (asked[:, k:k + 1] == spots).astype(F32)
                oht[k * 128:(k + 1) * 128, q * 512:(q + 1) * 512] = hit.astype(BF16)

    def gather(snd):
        high, low = split(grid[...])
        gmat[:, 0:128] = high
        gmat[:, 128:256] = low
        to_slots(oht, gmat, snd)

    table_of_asked()
    gather(snd3)
    first = dot3(amat[...], trans[...], BOTH)
    second = dot3(amat[...], first)
    arrived(0, rcv1, CAP)
    rows_in(rcv1)
    for q in range(4):
        rows_of = pl.ds(q * 512, 512)
        got = dot1(ohp[rows_of, :], zmat[...])
        place_rows(0, q, got[:, 0:128] + got[:, 128:256] + sc0[rows_of, :])

    lane = lax.broadcasted_iota(jnp.int32, (8, 128), 1)
    line = lax.broadcasted_iota(jnp.int32, (8, 128), 0)
    zero = jnp.zeros((8, 128), F32)
    tiles = lines // 8

    def sweep(number):
        src = field.at[number]
        last = number + 1 == 2 * SWEEPS

        def tile(at_z, t, h):
            return src[at_z, 8 * t + 8:8 * t + 16, 128 * h:128 * h + 128]

        def strip(z, which):
            for t in which:
                left, right = tile(z, t, 0), tile(z, t, 1)
                before_x = (jnp.where(lane == 127, zero, left), jnp.where(lane == 127, left, right))
                after_x = (jnp.where(lane == 0, right, left), jnp.where(lane == 0, zero, right))
                for h, mid in enumerate((left, right)):
                    x = slice(128 * h, 128 * h + 128)
                    total = tile(z - 1, t, h) + tile(z + 1, t, h)
                    total = total + feed[number // SWEEPS, z - 1, 8 * t:8 * t + 8, x]
                    total = total + (
                        pltpu.roll(jnp.where(line == 7, tile(z, t - 1, h), mid), 1, 0)
                        + pltpu.roll(jnp.where(line == 0, tile(z, t + 1, h), mid), 7, 0)
                    )
                    total = total + (
                        pltpu.roll(before_x[h], 1, 1) + pltpu.roll(after_x[h], 127, 1)
                    )
                    if last:
                        pot_out[z - 1, 8 * t:8 * t + 8, x] = total * scale
                    else:
                        field[number + 1, z, 8 * t + 8:8 * t + 16, x] = total * scale

        def over(first, count, step, which):
            def body(i, carry):
                strip(first + i * step, which)
                return carry

            lax.fori_loop(0, count, body, 0)

        halo(number, "recv")
        if last:
            over(1, depth, 1, range(tiles))
        else:
            over(1, 2, depth - 1, range(tiles))
            over(2, depth - 2, 1, (0, tiles - 1))
            halo(number + 1, "start")
            over(2, depth - 2, 1, range(1, tiles - 1))

    def bring(number, rcv):
        arrived(number, rcv, CAP)
        for k in range(CAP):
            high, low = split(jnp.transpose(rcv[pl.ds(k, DEVS, stride=SLOT), :]))
            lt[0:128, k * 128:(k + 1) * 128] = high
            lt[128:256, k * 128:(k + 1) * 128] = low
        got = dot1(lt[...], ohc[...])
        return got[0:128, :] + got[128:256, :]

    sweep(0)
    send_part(1, snd2, rcv2, CAP, 3, 4)
    ymat[...] = dot3(amat[...], volt[...])
    sweep(1)
    send_part(2, snd3, rcv3, CAP, 0, 1)
    ymat[...] = dot3(amat[...], ymat[...])
    sweep(2)
    send_part(2, snd3, rcv3, CAP, 1, 2)
    sweep(3)
    send_part(2, snd3, rcv3, CAP, 2, 4)
    for z in range(depth):
        now = field[SWEEPS, 1 + z, 8:8 + lines, :]
        grid[z * lines:(z + 1) * lines, :] = now[:, 0:128]
        grid[half + z * lines:half + (z + 1) * lines, :] = now[:, 128:256]
    for q in range(4):
        rows_of = pl.ds(q * 512, 512)
        se0[rows_of, :] = cnt[rows_of, :] * (
            se0[rows_of, :] + dot3(grid[rows_of, :], coef[0:128, :], BOTH)
        )
    arrived(1, rcv2, CAP)
    rows_in(rcv2)
    for q in range(4):
        rows_of = pl.ds(q * 512, 512)
        got = dot1(ohp[rows_of, :], zmat[...])
        place_rows(1, q, got[:, 0:128] + got[:, 128:256] + se0[rows_of, :])
    sweep(4)
    gather(snd4)
    send_part(3, snd4, rcv4, CAP, 0, 2)
    sweep(5)
    send_part(3, snd4, rcv4, CAP, 2, 3)
    volt_out[...] = ymat[...] + dot3(second, bring(2, rcv3))
    high, low = split(first)
    first_out[:, 0:128] = high
    first_out[:, 128:256] = high
    first_out[:, 256:384] = low
    sweep(6)
    send_part(3, snd4, rcv4, CAP, 3, 4)
    sweep(7)
    high, low = split(bring(3, rcv4))
    seen_out[0:128, :] = high
    seen_out[128:256, :] = low
    seen_out[256:384, :] = high
    departed(0, snd1, CAP)
    departed(4, sndi, 1)
    departed(1, snd2, CAP)
    departed(2, snd3, CAP)
    departed(3, snd4, CAP)
    for number in range(2 * SWEEPS):
        halo(number, "sent")


def shards(voltage, potential, transfer, conductance, inverses, parents, target, place):
    cells = voltage.shape[1]
    depth, lines, wide = potential.shape
    tall = (2 * SWEEPS, depth + 2, lines + 16, wide)
    vmem = pl.BlockSpec(memory_space=pltpu.VMEM)
    block = pltpu.VMEM((DEVS * SLOT, 128), F32)
    held, potential, first, seen = pl.pallas_call(
        kernel,
        out_shape=(
            jax.ShapeDtypeStruct(voltage.shape, F32),
            jax.ShapeDtypeStruct(potential.shape, F32),
            jax.ShapeDtypeStruct((512, 384), BF16),
            jax.ShapeDtypeStruct((384, cells), BF16),
        ),
        in_specs=[vmem] * 8,
        out_specs=(vmem,) * 4,
        scratch_shapes=[
            pltpu.VMEM((CAP * DEVS, cells), BF16),
            pltpu.VMEM((depth * lines * 2, CAP * DEVS), BF16),
            pltpu.VMEM((CAP * DEVS, depth * lines * 2), BF16),
            pltpu.VMEM((depth * lines * 2, 256), BF16),
            pltpu.VMEM((512, 512), F32),
            pltpu.VMEM((512, cells), F32),
            pltpu.VMEM((256, 128), F32),
            pltpu.VMEM((cells, 256), BF16),
            pltpu.VMEM((CAP * DEVS, 256), BF16),
            pltpu.VMEM((256, CAP * DEVS), BF16),
            pltpu.VMEM((depth * lines * 2, 128), F32),
            pltpu.VMEM((depth * lines * 2, 128), F32),
            pltpu.VMEM((depth * lines * 2, 128), F32),
            pltpu.VMEM((depth * lines * 2, 128), F32),
        ]
        + [pltpu.VMEM((DEVS * 8, 128), F32)] * 2
        + [block] * 8
        + [pltpu.VMEM(tall, F32), pltpu.VMEM((2, depth, lines, wide), F32)]
        + [
            pltpu.SemaphoreType.DMA((5,)),
            pltpu.SemaphoreType.DMA((5,)),
            pltpu.SemaphoreType.DMA((32,)),
            pltpu.SemaphoreType.DMA((32,)),
        ],
        compiler_params=pltpu.CompilerParams(
            collective_id=0, has_side_effects=True, vmem_limit_bytes=60 * 1024 * 1024
        ),
    )(
        voltage, potential, transfer, conductance.reshape(1, -1), inverses, parents.reshape(1, -1),
        target.reshape(1, -1), place,
    )
    voltage = held + dot1(first, seen)
    return voltage, potential


def solution(mesh):
    return jax.shard_map(
        shards,
        mesh=mesh,
        in_specs=(
            P(None, ("slab", "row")),
            P("slab", "row", None),
            P(),
            P(),
            P(),
            P(),
            P(("slab", "row"), None),
            P(("slab", "row")),
        ),
        out_specs=(P(None, ("slab", "row")), P("slab", "row", None)),
        check_vma=False,
    )
```
